8 devices in a mesh: dp: 1 (over z), tp: 8 (over x, y, core).
Axes of the slice: x: 2, y: 2, z: 1, core: 2. Of those that a mesh axis runs over, the one named last changes fastest.
Arguments:
- x: bfloat16 [2560, 3584], P(('dp', 'tp'))
- dy: bfloat16 [2560, 3584], P(('dp', 'tp'))
- gate: bfloat16 [2560, 14336], P('dp', 'tp')
- up: bfloat16 [2560, 14336], P('dp', 'tp')
- w_gate: bfloat16 [3584, 14336], P(None, 'tp')
- w_up: bfloat16 [3584, 14336], P(None, 'tp')
- w_down: bfloat16 [14336, 3584], P('tp')
Outputs:
- output 1: bfloat16 [2560, 3584], P(('dp', 'tp'))
- output 2: bfloat16 [3584, 14336], P('dp', 'tp')
- output 3: bfloat16 [3584, 14336], P('dp', 'tp')
- output 4: bfloat16 [14336, 3584], P(('dp', 'tp'))
All inputs are finite; a program needn't handle non-finite values.
Results may differ from the reference program's by a relative error of at most 0.012.
Values are sent between devices in bfloat16 or wider.
A program may use at most 2 GiB of HBM per device.

```python
import jax
import jax.numpy as jnp

ROWS = 2560
D = 3584
FF = 14336


def act(gate, up):
    return jax.nn.gelu(gate) * up


def setup_inputs(seed: int = 0, part: int = 0) -> dict:
    kx, ky, ka, kb, kg, ku, kd = jax.random.split(jax.random.key(seed), 7)
    kx, ky, ka, kb = (jax.random.fold_in(k, part) for k in (kx, ky, ka, kb))
    drawn = {
        "x": jax.random.normal(kx, (ROWS, D), jnp.float32),
        "dy": jax.random.normal(ky, (ROWS, D), jnp.float32),
        "gate": jax.random.normal(ka, (ROWS, FF), jnp.float32),
        "up": jax.random.normal(kb, (ROWS, FF), jnp.float32),
        "w_gate": jax.random.normal(kg, (D, FF), jnp.float32) * D**-0.5,
        "w_up": jax.random.normal(ku, (D, FF), jnp.float32) * D**-0.5,
        "w_down": jax.random.normal(kd, (FF, D), jnp.float32) * FF**-0.5,
    }
    return {k: v.astype(jnp.bfloat16) for k, v in drawn.items()}


def reference(x, dy, gate, up, w_gate, w_up, w_down):
    hidden, back = jax.vjp(act, gate.astype(jnp.float32), up.astype(jnp.float32))
    d_hidden = jnp.dot(dy, w_down.T, preferred_element_type=jnp.float32)
    d_gate, d_up = (g.astype(jnp.bfloat16) for g in back(d_hidden))
    dx = jnp.dot(d_gate, w_gate.T, preferred_element_type=jnp.float32) + jnp.dot(d_up, w_up.T, preferred_element_type=jnp.float32)
    dw_gate = jnp.dot(x.T, d_gate, preferred_element_type=jnp.float32)
    dw_up = jnp.dot(x.T, d_up, preferred_element_type=jnp.float32)
    dw_down = jnp.dot(hidden.astype(jnp.bfloat16).T, dy, preferred_element_type=jnp.float32)
    return tuple(g.astype(jnp.bfloat16) for g in (dx, dw_gate, dw_up, dw_down))
```

```python
import functools

import jax
import jax.numpy as jnp
from jax import lax
from jax.experimental import pallas as pl
from jax.experimental.pallas import tpu as pltpu
from jax.sharding import PartitionSpec as P

MESH = pl.DeviceIdType.MESH
ANY = pl.BlockSpec(memory_space=pl.ANY)
VMEM_LIMIT = 60 * 2**20
C0 = 0.7978845608028654
C1 = C0 * 0.044715


def act_and_back(gate, up, d_hidden):
    g = gate.astype(jnp.float32)
    u = up.astype(jnp.float32)
    g2 = g * g
    t = jnp.tanh(g * (C0 + C1 * g2))
    cdf = 0.5 + 0.5 * t
    gelu = g * cdf
    slope = cdf + (0.5 * g) * (1.0 - t * t) * (C0 + (3.0 * C1) * g2)
    return gelu * u, d_hidden * u * slope, d_hidden * gelu


def nt(a, b):
    return lax.dot_general(a, b, (((1,), (1,)), ((), ())), preferred_element_type=jnp.float32)


def tn(a, b):
    return lax.dot_general(a, b, (((0,), (0,)), ((), ())), preferred_element_type=jnp.float32)


def act_body(dy_ref, wd_ref, gate_ref, up_ref, dg_ref, du_ref, h_ref):
    d_hidden = nt(dy_ref[...], wd_ref[...])
    h, dg, du = act_and_back(gate_ref[...], up_ref[...], d_hidden)
    dg_ref[...] = dg.astype(jnp.bfloat16)
    du_ref[...] = du.astype(jnp.bfloat16)
    h_ref[...] = h.astype(jnp.bfloat16)


def dx_body(dg_ref, du_ref, wg_ref, wu_ref, o_ref):
    o_ref[...] = (nt(dg_ref[...], wg_ref[...]) + nt(du_ref[...], wu_ref[...])).astype(jnp.bfloat16)


def front_kernel(
    dy_ref, x_ref, gate_ref, up_ref, wd_ref, wg_ref, wu_ref,
    dyf_ref, xf_ref, dg_ref, du_ref, h_ref, dxp_ref,
    bounce, send_sem, recv_sem, local_sem,
):
    rows, d = dy_ref.shape
    half = rows // 2
    chunk = 2 * rows
    ff = wd_ref.shape[0]
    me = lax.axis_index("tp")
    core = me % 2
    other = me + 1 - 2 * core
    near_y = me + 2 - 4 * ((me // 2) % 2)
    near_x = me + 4 - 8 * (me // 4)
    far = near_y + 4 - 8 * (near_y // 4)

    barrier = pltpu.get_barrier_semaphore()
    for peer in (other, near_y, near_x):
        pl.semaphore_signal(barrier, inc=1, device_id={"tp": peer}, device_id_type=MESH)
    pl.semaphore_wait(barrier, 3)

    def block(owner, part=None):
        if part is None:
            return pl.ds(pl.multiple_of(owner * rows, rows), rows)
        return pl.ds(pl.multiple_of(owner * rows + part * half, half), half)

    class Gather:
        def __init__(self, a, own, full):
            self.a, self.own, self.full = a, own, full
            self.copies = {}

        def send(self, number, src, where, peer):
            copy = pltpu.make_async_remote_copy(
                src_ref=src,
                dst_ref=self.full.at[where, :],
                send_sem=send_sem.at[self.a, number],
                recv_sem=recv_sem.at[self.a, number],
                device_id={"tp": peer},
                device_id_type=MESH,
            )
            copy.start()
            self.copies[number] = copy

        def send_own(self, number, part, peer):
            src = self.own if part is None else self.own.at[pl.ds(part * half, half), :]
            self.send(number, src, block(me, part), peer)

        def pass_on(self, number, owner, part, peer):
            where = block(owner, part)
            self.send(number, self.full.at[where, :], where, peer)

        def arrived(self, *numbers):
            for number in numbers:
                self.copies[number].wait_recv()

        def start(self):
            self.send_own(1, 0, near_x)
            self.send_own(4, 1, near_y)
            self.send_own(2, 1, near_x)
            self.send_own(3, 0, near_y)
            self.send_own(0, None, other)

        def keep_own(self):
            into = pltpu.make_async_copy(self.own, bounce, local_sem.at[self.a, 0])
            into.start()
            into.wait()
            out = pltpu.make_async_copy(bounce, self.full.at[block(me), :], local_sem.at[self.a, 1])
            out.start()
            out.wait()

        def first(self):
            self.arrived(1, 4)
            self.pass_on(5, near_x, 0, near_y)
            self.pass_on(6, near_y, 1, near_x)
            self.pass_on(7, near_x, 0, other)
            self.pass_on(10, near_y, 1, other)

        def second(self):
            self.arrived(2, 3)
            self.pass_on(8, near_x, 1, other)
            self.pass_on(9, near_y, 0, other)

        def third(self):
            self.arrived(5, 6)
            self.pass_on(11, far, 0, other)
            self.pass_on(12, far, 1, other)

        def finish(self):
            for copy in self.copies.values():
                copy.wait_send()

    def rows_of(owner):
        return pl.ds(pl.multiple_of((owner // 2) * chunk, chunk), chunk)

    def act(owner):
        where = rows_of(owner)
        pltpu.emit_pipeline(
            act_body,
            grid=(ff // 256,),
            in_specs=[
                pl.BlockSpec((chunk, d), lambda n: (0, 0)),
                pl.BlockSpec((256, d), lambda n: (n, 0)),
                pl.BlockSpec((chunk, 256), lambda n: (0, n)),
                pl.BlockSpec((chunk, 256), lambda n: (0, n)),
            ],
            out_specs=[pl.BlockSpec((chunk, 256), lambda n: (0, n))] * 3,
        )(
            dyf_ref.at[where, :], wd_ref, gate_ref.at[where, :], up_ref.at[where, :],
            dg_ref.at[where, :], du_ref.at[where, :], h_ref.at[where, :],
        )

    def dx(owner):
        where = rows_of(owner)
        pltpu.emit_pipeline(
            dx_body,
            grid=(d // 512,),
            in_specs=[
                pl.BlockSpec((chunk, ff), lambda n: (0, 0)),
                pl.BlockSpec((chunk, ff), lambda n: (0, 0)),
                pl.BlockSpec((512, ff), lambda n: (n, 0)),
                pl.BlockSpec((512, ff), lambda n: (n, 0)),
            ],
            out_specs=[pl.BlockSpec((chunk, 512), lambda n: (0, n))],
        )(dg_ref.at[where, :], du_ref.at[where, :], wg_ref, wu_ref, dxp_ref.at[where, :])

    dys, xs = Gather(0, dy_ref, dyf_ref), Gather(1, x_ref, xf_ref)
    dys.start()
    dys.keep_own()
    dys.arrived(0)
    act(me)
    dx(me)
    dys.first()
    xs.start()
    dys.second()
    xs.keep_own()
    dys.arrived(7, 8, 9, 10)
    act(near_x)
    act(near_y)
    dys.third()
    dx(near_x)
    dys.arrived(11, 12)
    xs.first()
    act(far)
    dx(near_y)
    xs.second()
    dx(far)
    xs.third()
    xs.arrived(0, 7, 8, 9, 10, 11, 12)
    dys.finish()
    xs.finish()


def front(dy, x, gate, up, wd, wg, wu):
    rows, d = dy.shape
    tokens, ff = gate.shape
    bf16 = jnp.bfloat16
    return pl.pallas_call(
        front_kernel,
        out_shape=[
            jax.ShapeDtypeStruct((tokens, d), bf16),
            jax.ShapeDtypeStruct((tokens, d), bf16),
            jax.ShapeDtypeStruct((tokens, ff), bf16),
            jax.ShapeDtypeStruct((tokens, ff), bf16),
            jax.ShapeDtypeStruct((tokens, ff), bf16),
            jax.ShapeDtypeStruct((tokens, d), bf16),
        ],
        in_specs=[ANY] * 7,
        out_specs=[ANY] * 6,
        scratch_shapes=[
            pltpu.VMEM((rows, d), bf16),
            pltpu.SemaphoreType.DMA((2, 13)),
            pltpu.SemaphoreType.DMA((2, 13)),
            pltpu.SemaphoreType.DMA((2, 2)),
        ],
        compiler_params=pltpu.CompilerParams(
            collective_id=0, has_side_effects=True, vmem_limit_bytes=VMEM_LIMIT
        ),
        cost_estimate=pl.CostEstimate(
            flops=6 * tokens * d * ff, bytes_accessed=300 * 2**20, transcendentals=tokens * ff
        ),
        name="front",
    )(dy, x, gate, up, wd, wg, wu)


def dw_kernel(a_ref, b_ref, o_ref):
    o_ref[...] = tn(a_ref[...], b_ref[...]).astype(o_ref.dtype)


def dw(a, b, tm, tn_):
    tokens, m = a.shape
    n = b.shape[1]
    return pl.pallas_call(
        dw_kernel,
        out_shape=jax.ShapeDtypeStruct((m, n), jnp.bfloat16),
        grid=(m // tm, n // tn_),
        in_specs=[
            pl.BlockSpec((tokens, tm), lambda i, j: (0, i)),
            pl.BlockSpec((tokens, tn_), lambda i, j: (0, j)),
        ],
        out_specs=pl.BlockSpec((tm, tn_), lambda i, j: (i, j)),
        compiler_params=pltpu.CompilerParams(
            dimension_semantics=("arbitrary", "arbitrary"), vmem_limit_bytes=VMEM_LIMIT
        ),
        cost_estimate=pl.CostEstimate(
            flops=2 * tokens * m * n, bytes_accessed=2 * (tokens * m + 2 * tokens * n + m * n), transcendentals=0
        ),
        name="dw",
    )(a, b)


def solution(mesh):
    def step(x, dy, gate, up, wg, wu, wd):
        dyf, xf, dg, du, h, dxp = front(dy, x, gate, up, wd, wg, wu)
        dx = lax.psum_scatter(dxp, "tp", scatter_dimension=0, tiled=True)
        dw_down = dw(h, dyf, 896, 512)
        dw_gate = dw(xf, dg, 512, 896)
        dw_up = dw(xf, du, 512, 896)
        return dx, dw_gate, dw_up, dw_down

    rows, cols, down = P(("dp", "tp"), None), P("dp", "tp"), P("tp", None)
    weight = P(None, "tp")
    return jax.shard_map(
        step,
        mesh=mesh,
        in_specs=(rows, rows, cols, cols, weight, weight, down),
        out_specs=(rows, cols, cols, P(("dp", "tp"), None)),
        check_vma=False,
    )
```

```python
import functools

import jax
import jax.numpy as jnp
from jax import lax
from jax.experimental import pallas as pl
from jax.experimental.pallas import tpu as pltpu
from jax.sharding import PartitionSpec as P

MESH = pl.DeviceIdType.MESH
ANY = pl.BlockSpec(memory_space=pl.ANY)
VMEM_LIMIT = 60 * 2**20
C0 = 0.7978845608028654
C1 = C0 * 0.044715


def act_and_back(gate, up, d_hidden):
    g = gate.astype(jnp.float32)
    u = up.astype(jnp.float32)
    g2 = g * g
    t = jnp.tanh(g * (C0 + C1 * g2))
    cdf = 0.5 + 0.5 * t
    gelu = g * cdf
    slope = cdf + (0.5 * g) * (1.0 - t * t) * (C0 + (3.0 * C1) * g2)
    return gelu * u, d_hidden * u * slope, d_hidden * gelu


def nt(a, b):
    return lax.dot_general(a, b, (((1,), (1,)), ((), ())), preferred_element_type=jnp.float32)


def tn(a, b):
    return lax.dot_general(a, b, (((0,), (0,)), ((), ())), preferred_element_type=jnp.float32)

TILE = 256
WTILE = 512


def front_kernel(
    dy_ref, x_ref, gate_ref, up_ref, wd_ref, wg_ref, wu_ref,
    dyf_ref, xf_ref, dg_ref, du_ref, h_ref, dwd_ref, give_ref, got_ref, keep_s_ref, keep_n_ref, send_x_ref, send_y_ref,
    dgc, duc, wbuf, send_sem, recv_sem, pair_send, pair_recv, w_sem, dy_sem, wd_sem, gu_sem, out_sem, own_sem,
):
    rows, d = dy_ref.shape
    half = rows // 2
    ff = wd_ref.shape[0]
    tiles, wtiles = ff // TILE, d // WTILE
    me = lax.axis_index("tp")
    other = me + 1 - 2 * (me % 2)
    near_y = me + 2 - 4 * ((me // 2) % 2)
    near_x = me + 4 - 8 * (me // 4)
    far = near_y + 4 - 8 * (near_y // 4)
    across = other - me

    barrier = pltpu.get_barrier_semaphore()
    for peer in (other, near_y, near_x):
        pl.semaphore_signal(barrier, inc=1, device_id={"tp": peer}, device_id_type=MESH)
    pl.semaphore_wait(barrier, 3)

    def block(owner, part=None):
        if part is None:
            return pl.ds(pl.multiple_of(owner * rows, rows), rows)
        return pl.ds(pl.multiple_of(owner * rows + part * half, half), half)

    routes = [
        (me, None, other),
        (me, 0, near_x), (me, 1, near_x), (me, 0, near_y), (me, 1, near_y),
        (near_x, 0, near_y), (near_y, 1, near_x),
        (near_x, 0, other), (near_x, 1, other), (near_y, 0, other), (near_y, 1, other),
        (far, 0, other), (far, 1, other),
    ]
    places = [block(owner, part) for owner, part, _ in routes]

    class Gather:
        def __init__(self, a, own, full):
            self.a, self.own, self.full = a, own, full

        def copy(self, number):
            _, part, peer = routes[number]
            if number < 5:
                src = self.own if part is None else self.own.at[pl.ds(part * half, half), :]
            else:
                src = self.full.at[places[number], :]
            return pltpu.make_async_remote_copy(
                src_ref=src,
                dst_ref=self.full.at[places[number], :],
                send_sem=send_sem.at[self.a, number],
                recv_sem=recv_sem.at[self.a, number],
                device_id={"tp": peer},
                device_id_type=MESH,
            )

        def send(self, *numbers):
            for number in numbers:
                self.copy(number).start()

        def arrived(self, *numbers):
            for number in numbers:
                self.copy(number).wait_recv()

        def finish(self):
            for number in range(len(routes)):
                self.copy(number).wait_send()

    dys, xs = Gather(0, dy_ref, dyf_ref), Gather(1, x_ref, xf_ref)

    def pair(p):
        return pltpu.make_async_remote_copy(
            src_ref=give_ref.at[p],
            dst_ref=got_ref.at[p],
            send_sem=pair_send.at[p],
            recv_sem=pair_recv.at[p],
            device_id={"tp": other},
            device_id_type=MESH,
        )

    pieces = [
        [(other, 0), (other, 1), (me, 0), (me, 1)],
        [(near_x + across, 0), (near_y + across, 1), (near_x, 0), (near_y, 1)],
        [(near_x + across, 1), (near_y + across, 0), (near_x, 1), (near_y, 0)],
        [(far + across, 0), (far + across, 1), (far, 0), (far, 1)],
    ]
    where = [[block(*piece) for piece in part] for part in pieces]

    def w_copies(tile, slot):
        at = pl.ds(pl.multiple_of(tile * WTILE, WTILE), WTILE)
        return [
            pltpu.make_async_copy(ref.at[at, :], wbuf.at[slot, i], w_sem.at[slot, i]) for i, ref in enumerate((wg_ref, wu_ref))
        ]

    def dx(k, last, parts, ins, outs, store, hook_at=None, hook=None):
        def body(step, *refs):
            n = step.index[0]
            slot = lax.rem(wtiles * k + n, 2)
            for copy in w_copies(n, slot):
                copy.wait()

            def ahead():
                for copy in w_copies(lax.rem(n + 1, wtiles), 1 - slot):
                    copy.start()

            if last:
                pl.when(n < wtiles - 1)(ahead)
            else:
                ahead()
            if hook is not None:
                pl.when(n == hook_at)(hook)
            sums = [
                nt(dgc[p, pl.ds(first, count), :], wbuf[slot, 0]) + nt(duc[p, pl.ds(first, count), :], wbuf[slot, 1])
                for p, first, count in parts
            ]
            store(sums, refs[: len(ins)], refs[len(ins) :])

        spec = pl.BlockSpec((rows, WTILE), lambda n: (0, n))
        pltpu.emit_pipeline(
            body, grid=(wtiles,), in_specs=[spec] * len(ins), out_specs=[spec] * len(outs), _explicit_indices=True
        )(*ins, *outs)

    def give(k, p, hook_at=None, hook=None):
        def store(sums, _, outs):
            outs[0][...] = sums[0].astype(jnp.bfloat16)

        dx(k, False, [(p, 0, rows)], [], [give_ref.at[p]], store, hook_at, hook)
        pair(p).start()

    def with_acts(dyc, wdb, gub, hc, acc):
        def dy_load(p, i):
            if p == 0 and i >= 2:
                src = dy_ref.at[pl.ds((i - 2) * half, half), :]
            else:
                src = dyf_ref.at[where[p][i], :]
            return pltpu.make_async_copy(src, dyc.at[p % 2, pl.ds(i * half, half), :], dy_sem.at[p % 2, i])

        def wd_copy(tile, slot):
            at = pl.ds(pl.multiple_of(tile * TILE, TILE), TILE)
            return pltpu.make_async_copy(wd_ref.at[at, :], wdb.at[slot], wd_sem.at[slot])

        def gu_copies(p, tile, slot):
            at = pl.ds(pl.multiple_of(tile * TILE, TILE), TILE)
            return [
                pltpu.make_async_copy(
                    ref.at[where[p][i], at], gub.at[slot, j, pl.ds(i * half, half), :], gu_sem.at[slot, j, i]
                )
                for j, ref in enumerate((gate_ref, up_ref))
                for i in range(4)
            ]

        def out_copies(p):
            full = ((dgc.at[p], dg_ref), (duc.at[p], du_ref), (hc, h_ref))
            return [
                pltpu.make_async_copy(src.at[pl.ds(i * half, half), :], ref.at[where[p][i], :], out_sem.at[j, i])
                for j, (src, ref) in enumerate(full)
                for i in range(4)
            ]

        def act(p):
            for i in range(4):
                dy_load(p, i).wait()
            if p > 0:
                for copy in out_copies(p - 1):
                    copy.wait()

            def product(slot):
                acc[...] = nt(dyc[p % 2], wdb[slot])

            def elementwise(n, slot):
                at = pl.ds(pl.multiple_of(n * TILE, TILE), TILE)
                h, dg, du = act_and_back(gub[slot, 0], gub[slot, 1], acc[...])
                dgc[p, :, at] = dg.astype(jnp.bfloat16)
                duc[p, :, at] = du.astype(jnp.bfloat16)
                hc[:, at] = h.astype(jnp.bfloat16)

            def fetch(n, ahead_gu):
                count = tiles * p + n
                wd_copy(n, lax.rem(count, 2)).wait()
                for copy in gu_copies(p, n, lax.rem(count, 3)):
                    copy.wait()
                if p < 3:
                    wd_copy(lax.rem(n + 1, tiles), lax.rem(count + 1, 2)).start()
                else:
                    pl.when(n < tiles - 1)(lambda: wd_copy(n + 1, lax.rem(count + 1, 2)).start())
                if ahead_gu:
                    for copy in gu_copies(p, n + 1, lax.rem(count + 1, 3)):
                        copy.start()

            fetch(jnp.int32(0), True)
            product((tiles * p) % 2)

            def later(n, carry):
                count = tiles * p + n
                fetch(n, False)

                @pl.when(n < tiles - 1)
                def _():
                    for copy in gu_copies(p, n + 1, lax.rem(count + 1, 3)):
                        copy.start()

                elementwise(n - 1, lax.rem(count - 1, 3))
                product(lax.rem(count, 2))
                return carry

            lax.fori_loop(1, tiles, later, 0)
            if p < 3:
                for copy in gu_copies(p + 1, 0, (tiles * (p + 1)) % 3):
                    copy.start()
            elementwise(tiles - 1, (tiles * (p + 1) - 1) % 3)
            for copy in out_copies(p):
                copy.start()

        def own_x(leg):
            hold = dyc.at[1, pl.ds(0, rows), :]
            src, dst = ((x_ref, hold), (hold, xf_ref.at[block(me), :]))[leg]
            return pltpu.make_async_copy(src, dst, own_sem.at[leg])

        def own_dy():
            return pltpu.make_async_copy(dyc.at[0, pl.ds(rows, rows), :], dyf_ref.at[block(me), :], own_sem.at[2])

        dys.send(0, 1, 4, 2, 3)
        dy_load(0, 2).start()
        dy_load(0, 3).start()
        wd_copy(0, 0).start()
        for copy in gu_copies(0, 0, 0):
            copy.start()
        own_x(0).start()
        for copy in w_copies(0, 0):
            copy.start()
        dys.arrived(0)
        dy_load(0, 0).start()
        dy_load(0, 1).start()
        act(0)
        own_dy().start()
        own_x(0).wait()
        own_x(1).start()

        def first_halves():
            dys.arrived(1, 4)
            dys.send(5, 6, 7, 10)
            xs.send(0, 1, 4, 2, 3)

        def store_s(sums, _, outs):
            outs[0][...] = sums[0].astype(jnp.bfloat16)
            outs[1][...] = sums[1]

        dx(0, False, [(0, 0, rows), (0, rows, rows)], [], [give_ref.at[0], keep_s_ref], store_s, 4, first_halves)
        pair(0).start()
        own_x(1).wait()
        dys.arrived(7, 10)
        for i in range(4):
            dy_load(1, i).start()
        act(1)
        dys.arrived(2, 3)
        dys.send(8, 9)
        give(1, 1)
        own_dy().wait()
        dys.arrived(8, 9)
        for i in range(4):
            dy_load(2, i).start()
        act(2)

        def far_halves():
            dys.arrived(5, 6)
            dys.send(11, 12)

        give(2, 2, 3, far_halves)
        dys.arrived(11, 12)
        for i in range(4):
            dy_load(3, i).start()
        act(3)
        give(3, 3)
        for copy in out_copies(3):
            copy.wait()

    pl.run_scoped(
        with_acts,
        pltpu.VMEM((2, 2 * rows, d), jnp.bfloat16),
        pltpu.VMEM((2, TILE, d), jnp.bfloat16),
        pltpu.VMEM((3, 2, 2 * rows, TILE), jnp.bfloat16),
        pltpu.VMEM((2 * rows, ff), jnp.bfloat16),
        pltpu.VMEM((2 * rows, TILE), jnp.float32),
    )

    xs.arrived(1, 4)
    xs.send(5, 6, 7, 10)

    def down(h_tile, dy_tile, o_ref):
        o_ref[...] = tn(h_tile[...], dy_tile[...]).astype(jnp.bfloat16)

    tokens = dyf_ref.shape[0]
    pltpu.emit_pipeline(
        down,
        grid=(ff // 896, d // 512),
        in_specs=[
            pl.BlockSpec((tokens, 896), lambda i, j: (0, i)),
            pl.BlockSpec((tokens, 512), lambda i, j: (0, j)),
        ],
        out_specs=[pl.BlockSpec((896, 512), lambda i, j: (i, j))],
    )(h_ref, dyf_ref, dwd_ref)

    xs.arrived(2, 3)
    xs.send(8, 9)
    for p in (1, 2, 3):
        pair(p).wait_recv()

    def store_kept(sums, gots, outs):
        near0, near1, far_sum = (s + g[...].astype(jnp.float32) for s, g in zip(sums, gots))
        to_x, to_y, kept = outs
        to_x[pl.ds(0, half), :] = near0[:half].astype(jnp.bfloat16)
        to_y[pl.ds(0, half), :] = near0[half:].astype(jnp.bfloat16)
        kept[...] = near1
        to_x[pl.ds(half, half), :] = far_sum[:half].astype(jnp.bfloat16)
        to_y[pl.ds(half, half), :] = far_sum[half:].astype(jnp.bfloat16)

    def far_x():
        xs.arrived(5, 6)
        xs.send(11, 12)

    dx(
        4, True, [(p, rows, rows) for p in (1, 2, 3)], [got_ref.at[p] for p in (1, 2, 3)],
        [send_x_ref, send_y_ref, keep_n_ref], store_kept, wtiles - 2, far_x,
    )
    xs.arrived(0, 7, 8, 9, 10, 11, 12)
    pair(0).wait_recv()
    for p in range(4):
        pair(p).wait_send()
    dys.finish()
    xs.finish()


def front(dy, x, gate, up, wd, wg, wu):
    rows, d = dy.shape
    tokens, ff = gate.shape
    bf16, f32 = jnp.bfloat16, jnp.float32
    shapes = [
        ((tokens, d), bf16), ((tokens, d), bf16), ((tokens, ff), bf16), ((tokens, ff), bf16), ((tokens, ff), bf16),
        ((ff, d), bf16), ((4, rows, d), bf16), ((4, rows, d), bf16), ((rows, d), f32), ((rows, d), f32),
        ((rows, d), bf16), ((rows, d), bf16),
    ]
    dma = pltpu.SemaphoreType.DMA
    return pl.pallas_call(
        front_kernel,
        out_shape=[jax.ShapeDtypeStruct(*s) for s in shapes],
        in_specs=[ANY] * 7,
        out_specs=[ANY] * len(shapes),
        scratch_shapes=[
            pltpu.VMEM((4, 2 * rows, ff), bf16),
            pltpu.VMEM((4, 2 * rows, ff), bf16),
            pltpu.VMEM((2, 2, WTILE, ff), bf16),
            dma((2, 13)), dma((2, 13)), dma((4,)), dma((4,)), dma((2, 2)),
            dma((2, 4)), dma((2,)), dma((3, 2, 4)), dma((3, 4)), dma((3,)),
        ],
        compiler_params=pltpu.CompilerParams(
            collective_id=0, has_side_effects=True, vmem_limit_bytes=VMEM_LIMIT
        ),
        cost_estimate=pl.CostEstimate(
            flops=8 * tokens * d * ff, bytes_accessed=300 * 2**20, transcendentals=tokens * ff
        ),
        name="front",
    )(dy, x, gate, up, wd, wg, wu)


def dw_kernel(a_ref, b_hbm, o_ref, b, sems):
    n = b.shape[1]
    cuts = [(j * 256, 256) for j in range(n // 256)]

    def load(j):
        at = pl.ds(cuts[j][0], cuts[j][1])
        return pltpu.make_async_copy(b_hbm.at[:, at], b.at[:, at], sems.at[j])

    @pl.when(pl.program_id(0) == 0)
    def _():
        for j in range(len(cuts)):
            load(j).start()
        for j, (first, count) in enumerate(cuts):
            load(j).wait()
            o_ref[:, first : first + count] = tn(a_ref[...], b[:, first : first + count]).astype(o_ref.dtype)

    @pl.when(pl.program_id(0) > 0)
    def _():
        o_ref[...] = tn(a_ref[...], b[...]).astype(o_ref.dtype)


def dw(a, b, tm=256):
    tokens, m = a.shape
    n = b.shape[1]
    return pl.pallas_call(
        dw_kernel,
        out_shape=jax.ShapeDtypeStruct((m, n), jnp.bfloat16),
        grid=(m // tm,),
        in_specs=[pl.BlockSpec((tokens, tm), lambda i: (0, i)), ANY],
        out_specs=pl.BlockSpec((tm, n), lambda i: (i, 0)),
        scratch_shapes=[pltpu.VMEM((tokens, n), jnp.bfloat16), pltpu.SemaphoreType.DMA((n // 256,))],
        compiler_params=pltpu.CompilerParams(dimension_semantics=("arbitrary",), vmem_limit_bytes=VMEM_LIMIT),
        cost_estimate=pl.CostEstimate(
            flops=2 * tokens * m * n, bytes_accessed=2 * (tokens * m + tokens * n + m * n), transcendentals=0
        ),
        name="dw",
    )(a, b)


def solution(mesh):
    devices = mesh.shape["tp"]
    to_x = [(i, i ^ 4) for i in range(devices)]
    to_y = [(i, i ^ 2) for i in range(devices)]

    def step(x, dy, gate, up, wg, wu, wd):
        bf16, f32 = jnp.bfloat16, jnp.float32
        half = x.shape[0] // 2
        _, xf, dg, du, _, dw_down, _, got, keep_s, keep_n, send_x, send_y = front(dy, x, gate, up, wd, wg, wu)
        from_x = lax.ppermute(send_x, "tp", to_x)
        from_y = lax.ppermute(send_y, "tp", to_y)
        dw_gate = dw(xf, dg)
        on_y = (keep_n[half:] + from_x[half:].astype(f32)).astype(bf16)
        on_x = (keep_n[:half] + from_y[half:].astype(f32)).astype(bf16)
        du, on_y, on_x = lax.optimization_barrier((du, on_y, on_x))
        last_y = lax.ppermute(on_y, "tp", to_y)
        last_x = lax.ppermute(on_x, "tp", to_x)
        dw_up = dw(xf, du)
        kept = keep_s + got[0].astype(f32)
        dx = jnp.concatenate(
            [
                kept[:half] + from_x[:half].astype(f32) + last_y.astype(f32),
                kept[half:] + from_y[:half].astype(f32) + last_x.astype(f32),
            ]
        ).astype(bf16)
        return dx, dw_gate, dw_up, dw_down

    rows, cols, down = P(("dp", "tp"), None), P("dp", "tp"), P("tp", None)
    weight = P(None, "tp")
    return jax.shard_map(
        step,
        mesh=mesh,
        in_specs=(rows, rows, cols, cols, weight, weight, down),
        out_specs=(rows, cols, cols, P(("dp", "tp"), None)),
        check_vma=False,
    )
```

```python
import jax
import jax.numpy as jnp
from jax import lax
from jax.experimental import pallas as pl
from jax.experimental.pallas import tpu as pltpu
from jax.sharding import PartitionSpec as P

MESH = pl.DeviceIdType.MESH
ANY = pl.BlockSpec(memory_space=pl.ANY)
VMEM_LIMIT = 60 * 2**20
C0 = 0.7978845608028654
C1 = C0 * 0.044715


def act_and_back(gate, up, d_hidden):
    g = gate.astype(jnp.float32)
    u = up.astype(jnp.float32)
    g2 = g * g
    t = jnp.tanh(g * (C0 + C1 * g2))
    cdf = 0.5 + 0.5 * t
    gelu = g * cdf
    slope = cdf + (0.5 * g) * (1.0 - t * t) * (C0 + (3.0 * C1) * g2)
    return gelu * u, d_hidden * u * slope, d_hidden * gelu


def nt(a, b):
    return lax.dot_general(a, b, (((1,), (1,)), ((), ())), preferred_element_type=jnp.float32)


def tn(a, b):
    return lax.dot_general(a, b, (((0,), (0,)), ((), ())), preferred_element_type=jnp.float32)

TILE = 256
WTILE = 512


def front_kernel(
    dy_ref, x_ref, gate_ref, up_ref, wd_ref, wg_ref, wu_ref,
    dyf_ref, xf_ref, dg_ref, du_ref, h_ref, dwd_ref, give_ref, got_ref, keep_s_ref, keep_n_ref, send_x_ref, send_y_ref,
    dgc, duc, wbuf, send_sem, recv_sem, pair_send, pair_recv, w_sem, dy_sem, wd_sem, gu_sem, out_sem, own_sem,
):
    rows, d = dy_ref.shape
    half = rows // 2
    ff = wd_ref.shape[0]
    tiles, wtiles = ff // TILE, d // WTILE
    me = lax.axis_index("tp")
    other = me + 1 - 2 * (me % 2)
    near_y = me + 2 - 4 * ((me // 2) % 2)
    near_x = me + 4 - 8 * (me // 4)
    far = near_y + 4 - 8 * (near_y // 4)
    across = other - me

    barrier = pltpu.get_barrier_semaphore()
    for peer in (other, near_y, near_x):
        pl.semaphore_signal(barrier, inc=1, device_id={"tp": peer}, device_id_type=MESH)
    pl.semaphore_wait(barrier, 3)

    def block(owner, part=None):
        if part is None:
            return pl.ds(pl.multiple_of(owner * rows, rows), rows)
        return pl.ds(pl.multiple_of(owner * rows + part * half, half), half)

    routes = [
        (me, None, other),
        (me, 0, near_x), (me, 1, near_x), (me, 0, near_y), (me, 1, near_y),
        (near_x, 0, near_y), (near_y, 1, near_x),
        (near_x, 0, other), (near_x, 1, other), (near_y, 0, other), (near_y, 1, other),
        (far, 0, other), (far, 1, other),
    ]
    places = [block(owner, part) for owner, part, _ in routes]

    class Gather:
        def __init__(self, a, own, full):
            self.a, self.own, self.full = a, own, full

        def copy(self, number):
            _, part, peer = routes[number]
            if number < 5:
                src = self.own if part is None else self.own.at[pl.ds(part * half, half), :]
            else:
                src = self.full.at[places[number], :]
            return pltpu.make_async_remote_copy(
                src_ref=src,
                dst_ref=self.full.at[places[number], :],
                send_sem=send_sem.at[self.a, number],
                recv_sem=recv_sem.at[self.a, number],
                device_id={"tp": peer},
                device_id_type=MESH,
            )

        def send(self, *numbers):
            for number in numbers:
                self.copy(number).start()

        def arrived(self, *numbers):
            for number in numbers:
                self.copy(number).wait_recv()

        def finish(self):
            for number in range(len(routes)):
                self.copy(number).wait_send()

    dys, xs = Gather(0, dy_ref, dyf_ref), Gather(1, x_ref, xf_ref)

    def pair(p):
        return pltpu.make_async_remote_copy(
            src_ref=give_ref.at[p],
            dst_ref=got_ref.at[p],
            send_sem=pair_send.at[p],
            recv_sem=pair_recv.at[p],
            device_id={"tp": other},
            device_id_type=MESH,
        )

    pieces = [
        [(other, 0), (other, 1), (me, 0), (me, 1)],
        [(near_x + across, 0), (near_y + across, 1), (near_x, 0), (near_y, 1)],
        [(near_x + across, 1), (near_y + across, 0), (near_x, 1), (near_y, 0)],
        [(far + across, 0), (far + across, 1), (far, 0), (far, 1)],
    ]
    where = [[block(*piece) for piece in part] for part in pieces]

    def w_copies(tile, slot):
        at = pl.ds(pl.multiple_of(tile * WTILE, WTILE), WTILE)
        return [
            pltpu.make_async_copy(ref.at[at, :], wbuf.at[slot, i], w_sem.at[slot, i]) for i, ref in enumerate((wg_ref, wu_ref))
        ]

    def dx(k, last, parts, ins, outs, store, hooks):
        def body(step, *refs):
            n = step.index[0]
            slot = lax.rem(wtiles * k + n, 2)
            for copy in w_copies(n, slot):
                copy.wait()

            def ahead():
                for copy in w_copies(lax.rem(n + 1, wtiles), 1 - slot):
                    copy.start()

            if last:
                pl.when(n < wtiles - 1)(ahead)
            else:
                ahead()
            for at, hook in hooks.items():
                pl.when(n == at)(hook)
            sums = [
                nt(dgc[p, pl.ds(first, count), :], wbuf[slot, 0]) + nt(duc[p, pl.ds(first, count), :], wbuf[slot, 1])
                for p, first, count in parts
            ]
            store(sums, refs[: len(ins)], refs[len(ins) :])

        spec = pl.BlockSpec((rows, WTILE), lambda n: (0, n))
        pltpu.emit_pipeline(
            body, grid=(wtiles,), in_specs=[spec] * len(ins), out_specs=[spec] * len(outs), _explicit_indices=True
        )(*ins, *outs)

    def give(k, p, hooks={}):
        def store(sums, _, outs):
            outs[0][...] = sums[0].astype(jnp.bfloat16)

        dx(k, False, [(p, 0, rows)], [], [give_ref.at[p]], store, hooks)
        pair(p).start()

    def with_acts(dyc, wdb, gub, hc):
        def dy_load(p, i):
            if p == 0 and i >= 2:
                src = dy_ref.at[pl.ds((i - 2) * half, half), :]
            else:
                src = dyf_ref.at[where[p][i], :]
            return pltpu.make_async_copy(src, dyc.at[pl.ds(i * half, half), :], dy_sem.at[i])

        def wd_copy(j):
            at = pl.ds(pl.multiple_of(j * TILE, TILE), TILE)
            return pltpu.make_async_copy(wd_ref.at[at, :], wdb.at[at, :], wd_sem.at[j])

        def gu_copies(p):
            return [
                pltpu.make_async_copy(ref.at[where[p][i], :], gub.at[j, pl.ds(i * half, half), :], gu_sem.at[j, i])
                for j, ref in enumerate((gate_ref, up_ref))
                for i in range(4)
            ]

        def out_copies(p):
            full = ((dgc.at[p], dg_ref), (duc.at[p], du_ref), (hc, h_ref))
            return [
                pltpu.make_async_copy(src.at[pl.ds(i * half, half), :], ref.at[where[p][i], :], out_sem.at[j, i])
                for j, (src, ref) in enumerate(full)
                for i in range(4)
            ]

        def act(p):
            for i in range(4):
                dy_load(p, i).wait()
            for copy in gu_copies(p):
                copy.wait()
            if p > 0:
                for copy in out_copies(p - 1):
                    copy.wait()

            def tile(j, carry):
                if p == 0:
                    wd_copy(j).wait()
                at = pl.ds(pl.multiple_of(j * TILE, TILE), TILE)
                d_hidden = nt(dyc[...], wdb[at, :])
                h, dg, du = act_and_back(gub[0, :, at], gub[1, :, at], d_hidden)
                dgc[p, :, at] = dg.astype(jnp.bfloat16)
                duc[p, :, at] = du.astype(jnp.bfloat16)
                hc[:, at] = h.astype(jnp.bfloat16)
                return carry

            lax.fori_loop(0, tiles, tile, 0)
            for copy in out_copies(p):
                copy.start()
            if p < 3:
                for copy in gu_copies(p + 1):
                    copy.start()

        def own_x(leg):
            hold = dgc.at[3, pl.ds(0, rows), :], duc.at[3, pl.ds(0, rows), :]
            cols = pl.ds(0, ff), pl.ds(ff, ff)
            return [
                pltpu.make_async_copy(
                    *((x_ref.at[:, cols[c]], hold[c]) if leg == 0 else (hold[c], xf_ref.at[block(me), cols[c]])),
                    own_sem.at[leg, c],
                )
                for c in range(2)
            ]

        def own_dy():
            return pltpu.make_async_copy(dyc.at[pl.ds(rows, rows), :], dyf_ref.at[block(me), :], own_sem.at[2, 0])

        dys.send(0, 1, 4, 2, 3)
        dy_load(0, 2).start()
        dy_load(0, 3).start()
        wd_copy(0).start()
        for copy in gu_copies(0):
            copy.start()
        for j in range(1, tiles):
            wd_copy(j).start()
        for copy in own_x(0):
            copy.start()
        for copy in w_copies(0, 0):
            copy.start()
        dys.arrived(0)
        dy_load(0, 0).start()
        dy_load(0, 1).start()
        act(0)
        own_dy().start()
        for copy in own_x(0):
            copy.wait()
        for copy in own_x(1):
            copy.start()

        def first_halves():
            dys.arrived(1, 4)
            dys.send(5, 6, 7, 10)
            xs.send(0, 1, 4, 2, 3)

        def load(p, *numbers):
            def then():
                dys.arrived(*numbers)
                for i in range(4):
                    dy_load(p, i).start()

            return then

        def load_first():
            own_dy().wait()
            for copy in own_x(1):
                copy.wait()
            load(1, 7, 10)()

        def store_s(sums, _, outs):
            outs[0][...] = sums[0].astype(jnp.bfloat16)
            outs[1][...] = sums[1]

        dx(
            0, False, [(0, 0, rows), (0, rows, rows)], [], [give_ref.at[0], keep_s_ref], store_s,
            {wtiles - 3: first_halves, wtiles - 1: load_first},
        )
        pair(0).start()
        act(1)
        dys.arrived(2, 3)
        dys.send(8, 9)
        give(1, 1, {wtiles - 1: load(2, 8, 9)})
        act(2)

        def far_halves():
            dys.arrived(5, 6)
            dys.send(11, 12)

        give(2, 2, {wtiles - 4: far_halves, wtiles - 1: load(3, 11, 12)})
        act(3)
        give(3, 3)
        for copy in out_copies(3):
            copy.wait()

    pl.run_scoped(
        with_acts,
        pltpu.VMEM((2 * rows, d), jnp.bfloat16),
        pltpu.VMEM((ff, d), jnp.bfloat16),
        pltpu.VMEM((2, 2 * rows, ff), jnp.bfloat16),
        pltpu.VMEM((2 * rows, ff), jnp.bfloat16),
    )

    xs.arrived(1, 4)
    xs.send(5, 6, 7, 10)

    def down(h_tile, dy_tile, o_ref):
        o_ref[...] = tn(h_tile[...], dy_tile[...]).astype(jnp.bfloat16)

    tokens = dyf_ref.shape[0]
    pltpu.emit_pipeline(
        down,
        grid=(ff // 896, d // 512),
        in_specs=[
            pl.BlockSpec((tokens, 896), lambda i, j: (0, i)),
            pl.BlockSpec((tokens, 512), lambda i, j: (0, j)),
        ],
        out_specs=[pl.BlockSpec((896, 512), lambda i, j: (i, j))],
    )(h_ref, dyf_ref, dwd_ref)

    xs.arrived(2, 3)
    xs.send(8, 9)
    for p in (1, 2, 3):
        pair(p).wait_recv()

    def store_kept(sums, gots, outs):
        near0, near1, far_sum = (s + g[...].astype(jnp.float32) for s, g in zip(sums, gots))
        to_x, to_y, kept = outs
        to_x[pl.ds(0, half), :] = near0[:half].astype(jnp.bfloat16)
        to_y[pl.ds(0, half), :] = near0[half:].astype(jnp.bfloat16)
        kept[...] = near1
        to_x[pl.ds(half, half), :] = far_sum[:half].astype(jnp.bfloat16)
        to_y[pl.ds(half, half), :] = far_sum[half:].astype(jnp.bfloat16)

    def far_x():
        xs.arrived(5, 6)
        xs.send(11, 12)

    dx(
        4, True, [(p, rows, rows) for p in (1, 2, 3)], [got_ref.at[p] for p in (1, 2, 3)],
        [send_x_ref, send_y_ref, keep_n_ref], store_kept, {wtiles - 2: far_x},
    )
    xs.arrived(0, 7, 8, 9, 10, 11, 12)
    pair(0).wait_recv()
    for p in range(4):
        pair(p).wait_send()
    dys.finish()
    xs.finish()


def front(dy, x, gate, up, wd, wg, wu):
    rows, d = dy.shape
    tokens, ff = gate.shape
    bf16, f32 = jnp.bfloat16, jnp.float32
    shapes = [
        ((tokens, d), bf16), ((tokens, d), bf16), ((tokens, ff), bf16), ((tokens, ff), bf16), ((tokens, ff), bf16),
        ((ff, d), bf16), ((4, rows, d), bf16), ((4, rows, d), bf16), ((rows, d), f32), ((rows, d), f32),
        ((rows, d), bf16), ((rows, d), bf16),
    ]
    dma = pltpu.SemaphoreType.DMA
    return pl.pallas_call(
        front_kernel,
        out_shape=[jax.ShapeDtypeStruct(*s) for s in shapes],
        in_specs=[ANY] * 7,
        out_specs=[ANY] * len(shapes),
        scratch_shapes=[
            pltpu.VMEM((4, 2 * rows, ff), bf16),
            pltpu.VMEM((4, 2 * rows, ff), bf16),
            pltpu.VMEM((2, 2, WTILE, ff), bf16),
            dma((2, 13)), dma((2, 13)), dma((4,)), dma((4,)), dma((2, 2)),
            dma((4,)), dma((7,)), dma((2, 4)), dma((3, 4)), dma((3, 2)),
        ],
        compiler_params=pltpu.CompilerParams(
            collective_id=0, has_side_effects=True, vmem_limit_bytes=VMEM_LIMIT
        ),
        cost_estimate=pl.CostEstimate(
            flops=8 * tokens * d * ff, bytes_accessed=300 * 2**20, transcendentals=tokens * ff
        ),
        name="front",
    )(dy, x, gate, up, wd, wg, wu)


def dw_kernel(a_ref, b_ref, o_ref):
    o_ref[...] = tn(a_ref[...], b_ref[...]).astype(o_ref.dtype)


def dw_kernel_and_move(a_ref, b_ref, src_ref, o_ref, dst_ref, hold, sems):
    i, steps = pl.program_id(0), pl.num_programs(0)
    count = hold.shape[1]

    def leg(out, k):
        at = pl.ds(pl.multiple_of(k * count, count), count)
        slot = lax.rem(k, 2)
        pair = (hold.at[slot], dst_ref.at[at, :]) if out else (src_ref.at[at, :], hold.at[slot])
        return pltpu.make_async_copy(*pair, sems.at[out, slot])

    @pl.when(i > 0)
    def _():
        leg(0, i - 1).wait()
        leg(1, i - 1).start()

    @pl.when(i > 1)
    def _():
        leg(1, i - 2).wait()

    leg(0, i).start()
    o_ref[...] = tn(a_ref[...], b_ref[...]).astype(o_ref.dtype)

    @pl.when(i == steps - 1)
    def _():
        leg(0, i).wait()
        leg(1, i).start()
        leg(1, i - 1).wait()
        leg(1, i).wait()


def dw(a, b, moved=None, tm=512):
    tokens, m = a.shape
    n = b.shape[1]
    steps = m // tm
    bf16 = jnp.bfloat16
    specs = [
        pl.BlockSpec((tokens, tm), lambda i: (0, i)),
        pl.BlockSpec((tokens, n), lambda i: (0, 0), pipeline_mode=pl.Buffered(1)),
    ]
    out, out_spec = jax.ShapeDtypeStruct((m, n), bf16), pl.BlockSpec((tm, n), lambda i: (i, 0))
    common = dict(
        grid=(steps,),
        compiler_params=pltpu.CompilerParams(dimension_semantics=("arbitrary",), vmem_limit_bytes=VMEM_LIMIT),
        cost_estimate=pl.CostEstimate(
            flops=2 * tokens * m * n, bytes_accessed=2 * (tokens * m + tokens * n + m * n), transcendentals=0
        ),
    )
    if moved is None:
        return pl.pallas_call(dw_kernel, out_shape=out, in_specs=specs, out_specs=out_spec, name="dw", **common)(a, b)
    return pl.pallas_call(
        dw_kernel_and_move,
        out_shape=[out, jax.ShapeDtypeStruct(moved.shape, bf16)],
        in_specs=specs + [ANY],
        out_specs=[out_spec, ANY],
        scratch_shapes=[
            pltpu.VMEM((2, moved.shape[0] // steps, moved.shape[1]), bf16),
            pltpu.SemaphoreType.DMA((2, 2)),
        ],
        name="dw_and_move",
        **common,
    )(a, b, moved)


def solution(mesh):
    devices = mesh.shape["tp"]
    to_x = [(i, i ^ 4) for i in range(devices)]
    to_y = [(i, i ^ 2) for i in range(devices)]

    def step(x, dy, gate, up, wg, wu, wd):
        bf16, f32 = jnp.bfloat16, jnp.float32
        half = x.shape[0] // 2
        _, xf, dg, du, _, dw_down, _, got, keep_s, keep_n, send_x, send_y = front(dy, x, gate, up, wd, wg, wu)
        from_x = lax.ppermute(send_x, "tp", to_x)
        from_y = lax.ppermute(send_y, "tp", to_y)
        dw_gate, dw_down = dw(xf, dg, dw_down)
        on_y = (keep_n[half:] + from_x[half:].astype(f32)).astype(bf16)
        on_x = (keep_n[:half] + from_y[half:].astype(f32)).astype(bf16)
        du, on_y, on_x = lax.optimization_barrier((du, on_y, on_x))
        last_y = lax.ppermute(on_y, "tp", to_y)
        last_x = lax.ppermute(on_x, "tp", to_x)
        dw_up = dw(xf, du)
        keep_s, got, last_y, last_x = lax.optimization_barrier((keep_s, got, last_y, last_x))
        kept = keep_s + got[0].astype(f32)
        dx = jnp.concatenate(
            [
                kept[:half] + from_x[:half].astype(f32) + last_y.astype(f32),
                kept[half:] + from_y[:half].astype(f32) + last_x.astype(f32),
            ]
        ).astype(bf16)
        return dx, dw_gate, dw_up, dw_down

    rows, cols, down = P(("dp", "tp"), None), P("dp", "tp"), P("tp", None)
    weight = P(None, "tp")
    return jax.shard_map(
        step,
        mesh=mesh,
        in_specs=(rows, rows, cols, cols, weight, weight, down),
        out_specs=(rows, cols, cols, P(("dp", "tp"), None)),
        check_vma=False,
    )
```

```python
import jax
import jax.numpy as jnp
from jax import lax
from jax.experimental import pallas as pl
from jax.experimental.pallas import tpu as pltpu
from jax.sharding import PartitionSpec as P

MESH = pl.DeviceIdType.MESH
ANY = pl.BlockSpec(memory_space=pl.ANY)
VMEM_LIMIT = 60 * 2**20
C0 = 0.7978845608028654
C1 = C0 * 0.044715


def act_and_back(gate, up, d_hidden):
    g = gate.astype(jnp.float32)
    u = up.astype(jnp.float32)
    g2 = g * g
    t = jnp.tanh(g * (C0 + C1 * g2))
    cdf = 0.5 + 0.5 * t
    gelu = g * cdf
    slope = cdf + (0.5 * g) * (1.0 - t * t) * (C0 + (3.0 * C1) * g2)
    return gelu * u, d_hidden * u * slope, d_hidden * gelu


def nt(a, b):
    return lax.dot_general(a, b, (((1,), (1,)), ((), ())), preferred_element_type=jnp.float32)


def tn(a, b):
    return lax.dot_general(a, b, (((0,), (0,)), ((), ())), preferred_element_type=jnp.float32)

TILE = 256
WTILE = 512


def front_kernel(
    dy_ref, x_ref, gate_ref, up_ref, wd_ref, wg_ref, wu_ref,
    dyf_ref, xf_ref, dg_ref, du_ref, h_ref, give_ref, got_ref, keep_s_ref, keep_n_ref, send_x_ref, send_y_ref,
    dgc, duc, wbuf, send_sem, recv_sem, pair_send, pair_recv, w_sem, dy_sem, wd_sem, gu_sem, out_sem, own_sem,
):
    rows, d = dy_ref.shape
    half = rows // 2
    ff = wd_ref.shape[0]
    tiles, wtiles = ff // TILE, d // WTILE
    me = lax.axis_index("tp")
    other = me + 1 - 2 * (me % 2)
    near_y = me + 2 - 4 * ((me // 2) % 2)
    near_x = me + 4 - 8 * (me // 4)
    far = near_y + 4 - 8 * (near_y // 4)
    across = other - me

    barrier = pltpu.get_barrier_semaphore()
    for peer in (other, near_y, near_x):
        pl.semaphore_signal(barrier, inc=1, device_id={"tp": peer}, device_id_type=MESH)
    pl.semaphore_wait(barrier, 3)

    def block(owner, part=None):
        if part is None:
            return pl.ds(pl.multiple_of(owner * rows, rows), rows)
        return pl.ds(pl.multiple_of(owner * rows + part * half, half), half)

    routes = [
        (me, None, other),
        (me, 0, near_x), (me, 1, near_x), (me, 0, near_y), (me, 1, near_y),
        (near_x, 0, near_y), (near_y, 1, near_x),
        (near_x, 0, other), (near_x, 1, other), (near_y, 0, other), (near_y, 1, other),
        (far, 0, other), (far, 1, other),
    ]
    places = [block(owner, part) for owner, part, _ in routes]

    class Gather:
        def __init__(self, a, own, full):
            self.a, self.own, self.full = a, own, full

        def copy(self, number):
            _, part, peer = routes[number]
            if number < 5:
                src = self.own if part is None else self.own.at[pl.ds(part * half, half), :]
            else:
                src = self.full.at[places[number], :]
            return pltpu.make_async_remote_copy(
                src_ref=src,
                dst_ref=self.full.at[places[number], :],
                send_sem=send_sem.at[self.a, number],
                recv_sem=recv_sem.at[self.a, number],
                device_id={"tp": peer},
                device_id_type=MESH,
            )

        def send(self, *numbers):
            for number in numbers:
                self.copy(number).start()

        def arrived(self, *numbers):
            for number in numbers:
                self.copy(number).wait_recv()

        def finish(self):
            for number in range(len(routes)):
                self.copy(number).wait_send()

    dys, xs = Gather(0, dy_ref, dyf_ref), Gather(1, x_ref, xf_ref)

    def pair(p):
        return pltpu.make_async_remote_copy(
            src_ref=give_ref.at[p],
            dst_ref=got_ref.at[p],
            send_sem=pair_send.at[p],
            recv_sem=pair_recv.at[p],
            device_id={"tp": other},
            device_id_type=MESH,
        )

    pieces = [
        [(other, 0), (other, 1), (me, 0), (me, 1)],
        [(near_x + across, 0), (near_y + across, 1), (near_x, 0), (near_y, 1)],
        [(near_x + across, 1), (near_y + across, 0), (near_x, 1), (near_y, 0)],
        [(far + across, 0), (far + across, 1), (far, 0), (far, 1)],
    ]
    where = [[block(*piece) for piece in part] for part in pieces]

    def w_copies(tile, slot):
        at = pl.ds(pl.multiple_of(tile * WTILE, WTILE), WTILE)
        return [
            pltpu.make_async_copy(ref.at[at, :], wbuf.at[slot, i], w_sem.at[slot, i]) for i, ref in enumerate((wg_ref, wu_ref))
        ]

    def dx(k, last, parts, ins, outs, store, hooks, heights=None):
        def body(step, *refs):
            n = step.index[0]
            slot = lax.rem(wtiles * k + n, 2)
            for copy in w_copies(n, slot):
                copy.wait()

            def ahead():
                for copy in w_copies(lax.rem(n + 1, wtiles), 1 - slot):
                    copy.start()

            if last:
                pl.when(n < wtiles - 1)(ahead)
            else:
                ahead()
            for at, hook in hooks.items():
                pl.when(n == at)(hook)
            sums = [
                nt(dgc[p, pl.ds(first, count), :], wbuf[slot, 0]) + nt(duc[p, pl.ds(first, count), :], wbuf[slot, 1])
                for p, first, count in parts
            ]
            store(sums, refs[: len(ins)], refs[len(ins) :])

        def spec(height):
            return pl.BlockSpec((height, WTILE), lambda n: (0, n))

        pltpu.emit_pipeline(
            body,
            grid=(wtiles,),
            in_specs=[spec(rows) for _ in ins],
            out_specs=[spec(height) for height in heights or [rows] * len(outs)],
            _explicit_indices=True,
        )(*ins, *outs)

    def give(k, p, hooks={}):
        def store(sums, _, outs):
            outs[0][...] = sums[0].astype(jnp.bfloat16)

        dx(k, False, [(p, 0, rows)], [], [give_ref.at[p]], store, hooks)
        pair(p).start()

    def with_acts(dyc, wdb, gub, hc):
        def dy_load(p, i):
            if p == 0 and i >= 2:
                src = dy_ref.at[pl.ds((i - 2) * half, half), :]
            else:
                src = dyf_ref.at[where[p][i], :]
            return pltpu.make_async_copy(src, dyc.at[pl.ds(i * half, half), :], dy_sem.at[i])

        def wd_copy(j):
            at = pl.ds(pl.multiple_of(j * TILE, TILE), TILE)
            return pltpu.make_async_copy(wd_ref.at[at, :], wdb.at[at, :], wd_sem.at[j])

        def gu_copies(p):
            return [
                pltpu.make_async_copy(ref.at[where[p][i], :], gub.at[j, pl.ds(i * half, half), :], gu_sem.at[j, i])
                for j, ref in enumerate((gate_ref, up_ref))
                for i in range(4)
            ]

        def out_copies(p):
            full = ((dgc.at[p], dg_ref), (duc.at[p], du_ref), (hc, h_ref))
            return [
                pltpu.make_async_copy(src.at[pl.ds(i * half, half), :], ref.at[where[p][i], :], out_sem.at[j, i])
                for j, (src, ref) in enumerate(full)
                for i in range(4)
            ]

        def act(p):
            for i in range(4):
                dy_load(p, i).wait()
            for copy in gu_copies(p):
                copy.wait()
            if p > 0:
                for copy in out_copies(p - 1):
                    copy.wait()

            def tile(j, carry):
                if p == 0:
                    wd_copy(j).wait()
                at = pl.ds(pl.multiple_of(j * TILE, TILE), TILE)
                d_hidden = nt(dyc[...], wdb[at, :])
                h, dg, du = act_and_back(gub[0, :, at], gub[1, :, at], d_hidden)
                dgc[p, :, at] = dg.astype(jnp.bfloat16)
                duc[p, :, at] = du.astype(jnp.bfloat16)
                hc[:, at] = h.astype(jnp.bfloat16)
                return carry

            lax.fori_loop(0, tiles, tile, 0)
            for copy in out_copies(p):
                copy.start()
            if p < 3:
                for copy in gu_copies(p + 1):
                    copy.start()

        def own_x(leg):
            hold = dgc.at[3, pl.ds(0, rows), :], duc.at[3, pl.ds(0, rows), :]
            cols = pl.ds(0, ff), pl.ds(ff, ff)
            return [
                pltpu.make_async_copy(
                    *((x_ref.at[:, cols[c]], hold[c]) if leg == 0 else (hold[c], xf_ref.at[block(me), cols[c]])),
                    own_sem.at[leg, c],
                )
                for c in range(2)
            ]

        def own_dy():
            return pltpu.make_async_copy(dyc.at[pl.ds(rows, rows), :], dyf_ref.at[block(me), :], own_sem.at[2, 0])

        dys.send(0, 1, 4, 2, 3)
        dy_load(0, 2).start()
        dy_load(0, 3).start()
        wd_copy(0).start()
        for copy in gu_copies(0):
            copy.start()
        wd_copy(1).start()
        dys.arrived(0)
        dy_load(0, 0).start()
        dy_load(0, 1).start()
        for j in range(2, tiles):
            wd_copy(j).start()
        for copy in own_x(0):
            copy.start()
        for copy in w_copies(0, 0):
            copy.start()
        act(0)
        own_dy().start()
        for copy in own_x(0):
            copy.wait()
        for copy in own_x(1):
            copy.start()

        def first_halves():
            dys.arrived(1, 4)
            dys.send(5, 6, 7, 10)
            xs.send(0, 1, 4, 2, 3)

        def load(p, *numbers):
            def then():
                dys.arrived(*numbers)
                for i in range(4):
                    dy_load(p, i).start()

            return then

        def load_first():
            own_dy().wait()
            for copy in own_x(1):
                copy.wait()
            load(1, 7, 10)()

        def store_s(sums, _, outs):
            outs[0][...] = sums[0].astype(jnp.bfloat16)
            outs[1][...] = sums[1]

        dx(
            0, False, [(0, 0, rows), (0, rows, rows)], [], [give_ref.at[0], keep_s_ref], store_s,
            {wtiles - 3: first_halves, wtiles - 1: load_first},
        )
        pair(0).start()
        act(1)
        dys.arrived(2, 3)
        dys.send(8, 9)
        give(1, 1, {wtiles - 1: load(2, 8, 9)})
        act(2)

        def far_halves():
            dys.arrived(5, 6)
            dys.send(11, 12)

        give(2, 2, {wtiles - 4: far_halves, wtiles - 1: load(3, 11, 12)})
        act(3)
        give(3, 3)
        for copy in out_copies(3):
            copy.wait()

    pl.run_scoped(
        with_acts,
        pltpu.VMEM((2 * rows, d), jnp.bfloat16),
        pltpu.VMEM((ff, d), jnp.bfloat16),
        pltpu.VMEM((2, 2 * rows, ff), jnp.bfloat16),
        pltpu.VMEM((2 * rows, ff), jnp.bfloat16),
    )

    xs.arrived(1, 4)
    xs.send(5, 6, 7, 10)
    for p in (1, 2):
        pair(p).wait_recv()

    def second_halves():
        xs.arrived(2, 3)
        xs.send(8, 9)

    def store_near(sums, gots, outs):
        near0, near1 = (s + g[...].astype(jnp.float32) for s, g in zip(sums, gots))
        to_x, to_y, kept = outs
        to_x[...] = near0[:half].astype(jnp.bfloat16)
        to_y[...] = near0[half:].astype(jnp.bfloat16)
        kept[...] = near1

    dx(
        4, False, [(p, rows, rows) for p in (1, 2)], [got_ref.at[1], got_ref.at[2]],
        [send_x_ref.at[0], send_y_ref.at[0], keep_n_ref], store_near, {wtiles - 2: second_halves}, [half, half, rows],
    )
    pair(3).wait_recv()

    def store_far(sums, gots, outs):
        total = sums[0] + gots[0][...].astype(jnp.float32)
        outs[0][...] = total[:half].astype(jnp.bfloat16)
        outs[1][...] = total[half:].astype(jnp.bfloat16)

    dx(5, True, [(3, rows, rows)], [got_ref.at[3]], [send_x_ref.at[1], send_y_ref.at[1]], store_far, {}, [half, half])
    xs.arrived(5, 6)
    xs.send(11, 12)
    xs.arrived(0, 7, 8, 9, 10, 11, 12)
    pair(0).wait_recv()
    for p in range(4):
        pair(p).wait_send()
    dys.finish()
    xs.finish()


def front(dy, x, gate, up, wd, wg, wu):
    rows, d = dy.shape
    tokens, ff = gate.shape
    bf16, f32 = jnp.bfloat16, jnp.float32
    shapes = [
        ((tokens, d), bf16), ((tokens, d), bf16), ((tokens, ff), bf16), ((tokens, ff), bf16), ((tokens, ff), bf16),
        ((4, rows, d), bf16), ((4, rows, d), bf16), ((rows, d), f32), ((rows, d), f32),
        ((2, rows // 2, d), bf16), ((2, rows // 2, d), bf16),
    ]
    dma = pltpu.SemaphoreType.DMA
    return pl.pallas_call(
        front_kernel,
        out_shape=[jax.ShapeDtypeStruct(*s) for s in shapes],
        in_specs=[ANY] * 7,
        out_specs=[ANY] * len(shapes),
        scratch_shapes=[
            pltpu.VMEM((4, 2 * rows, ff), bf16),
            pltpu.VMEM((4, 2 * rows, ff), bf16),
            pltpu.VMEM((2, 2, WTILE, ff), bf16),
            dma((2, 13)), dma((2, 13)), dma((4,)), dma((4,)), dma((2, 2)),
            dma((4,)), dma((7,)), dma((2, 4)), dma((3, 4)), dma((3, 2)),
        ],
        compiler_params=pltpu.CompilerParams(
            collective_id=0, has_side_effects=True, vmem_limit_bytes=VMEM_LIMIT
        ),
        cost_estimate=pl.CostEstimate(
            flops=6 * tokens * d * ff, bytes_accessed=300 * 2**20, transcendentals=tokens * ff
        ),
        name="front",
    )(dy, x, gate, up, wd, wg, wu)


def dw_kernel(a_ref, b_ref, o_ref):
    o_ref[...] = tn(a_ref[...], b_ref[...]).astype(o_ref.dtype)


def dw(a, b, tm=512):
    tokens, m = a.shape
    n = b.shape[1]
    return pl.pallas_call(
        dw_kernel,
        out_shape=jax.ShapeDtypeStruct((m, n), jnp.bfloat16),
        grid=(m // tm,),
        in_specs=[
            pl.BlockSpec((tokens, tm), lambda i: (0, i)),
            pl.BlockSpec((tokens, n), lambda i: (0, 0), pipeline_mode=pl.Buffered(1)),
        ],
        out_specs=pl.BlockSpec((tm, n), lambda i: (i, 0)),
        compiler_params=pltpu.CompilerParams(dimension_semantics=("arbitrary",), vmem_limit_bytes=VMEM_LIMIT),
        cost_estimate=pl.CostEstimate(
            flops=2 * tokens * m * n, bytes_accessed=2 * (tokens * m + tokens * n + m * n), transcendentals=0
        ),
        name="dw",
    )(a, b)


def dw_two(h, dy, x, dg, tile=512):
    tokens, ff = h.shape
    d = dy.shape[1]
    steps = d // tile

    def kernel(h_ref, dy_ref, x_ref, dg_hbm, down_ref, gate_ref, held, sem):
        i = pl.program_id(0)
        load = pltpu.make_async_copy(dg_hbm, held, sem)

        @pl.when(i == 0)
        def _():
            load.start()

        @pl.when(i < steps)
        def _():
            down_ref[...] = tn(h_ref[...], dy_ref[...]).astype(down_ref.dtype)

        @pl.when(i == steps - 1)
        def _():
            load.wait()

        @pl.when(i >= steps)
        def _():
            gate_ref[...] = tn(x_ref[...], held[...]).astype(gate_ref.dtype)

    def first(i):
        return jnp.minimum(i, steps - 1)

    def second(i):
        return jnp.maximum(i - steps, 0)

    return pl.pallas_call(
        kernel,
        out_shape=[jax.ShapeDtypeStruct((ff, d), jnp.bfloat16), jax.ShapeDtypeStruct((d, ff), jnp.bfloat16)],
        grid=(2 * steps,),
        in_specs=[
            pl.BlockSpec((tokens, ff), lambda i: (0, 0), pipeline_mode=pl.Buffered(1)),
            pl.BlockSpec((tokens, tile), lambda i: (0, first(i))),
            pl.BlockSpec((tokens, tile), lambda i: (0, second(i))),
            ANY,
        ],
        out_specs=[
            pl.BlockSpec((ff, tile), lambda i: (0, first(i))),
            pl.BlockSpec((tile, ff), lambda i: (second(i), 0)),
        ],
        scratch_shapes=[pltpu.VMEM((tokens, ff), jnp.bfloat16), pltpu.SemaphoreType.DMA(())],
        compiler_params=pltpu.CompilerParams(dimension_semantics=("arbitrary",), vmem_limit_bytes=VMEM_LIMIT),
        cost_estimate=pl.CostEstimate(
            flops=4 * tokens * d * ff, bytes_accessed=4 * (tokens * d + tokens * ff + d * ff), transcendentals=0
        ),
        name="dw_two",
    )(h, dy, x, dg)


def sum_rows(kept, got, from_x, from_y, last_x, last_y, tile=896):
    rows, d = kept.shape
    half = rows // 2

    def kernel(kept_ref, got_ref, fx_ref, fy_ref, lx_ref, ly_ref, o_ref):
        f32 = jnp.float32
        for at, near, last in ((pl.ds(0, half), fx_ref, ly_ref), (pl.ds(half, half), fy_ref, lx_ref)):
            total = kept_ref[at, :] + got_ref[0, at, :].astype(f32) + near[0].astype(f32) + last[...].astype(f32)
            o_ref[at, :] = total.astype(o_ref.dtype)

    full = pl.BlockSpec((rows, tile), lambda i: (0, i))
    part = pl.BlockSpec((1, half, tile), lambda i: (0, 0, i))
    last = pl.BlockSpec((half, tile), lambda i: (0, i))
    return pl.pallas_call(
        kernel,
        out_shape=jax.ShapeDtypeStruct((rows, d), jnp.bfloat16),
        grid=(d // tile,),
        in_specs=[full, pl.BlockSpec((1, rows, tile), lambda i: (0, 0, i)), part, part, last, last],
        out_specs=full,
        compiler_params=pltpu.CompilerParams(dimension_semantics=("arbitrary",), vmem_limit_bytes=VMEM_LIMIT),
        cost_estimate=pl.CostEstimate(flops=4 * rows * d, bytes_accessed=14 * rows * d, transcendentals=0),
        name="sum_rows",
    )(kept, got, from_x, from_y, last_x, last_y)


def solution(mesh):
    devices = mesh.shape["tp"]
    to_x = [(i, i ^ 4) for i in range(devices)]
    to_y = [(i, i ^ 2) for i in range(devices)]

    def step(x, dy, gate, up, wg, wu, wd):
        bf16, f32 = jnp.bfloat16, jnp.float32
        half = x.shape[0] // 2
        dyf, xf, dg, du, h, _, got, keep_s, keep_n, send_x, send_y = front(dy, x, gate, up, wd, wg, wu)
        from_x = lax.ppermute(send_x, "tp", to_x)
        from_y = lax.ppermute(send_y, "tp", to_y)
        dw_down, dw_gate = dw_two(h, dyf, xf, dg)
        on_y = (keep_n[half:] + from_x[1].astype(f32)).astype(bf16)
        on_x = (keep_n[:half] + from_y[1].astype(f32)).astype(bf16)
        du, on_y, on_x = lax.optimization_barrier((du, on_y, on_x))
        last_y = lax.ppermute(on_y, "tp", to_y)
        last_x = lax.ppermute(on_x, "tp", to_x)
        dw_up = dw(xf, du)
        dx = sum_rows(keep_s, got, from_x, from_y, last_x, last_y)
        return dx, dw_gate, dw_up, dw_down

    rows, cols, down = P(("dp", "tp"), None), P("dp", "tp"), P("tp", None)
    weight = P(None, "tp")
    return jax.shard_map(
        step,
        mesh=mesh,
        in_specs=(rows, rows, cols, cols, weight, weight, down),
        out_specs=(rows, cols, cols, P(("dp", "tp"), None)),
        check_vma=False,
    )
```

```python
import jax
import jax.numpy as jnp
from jax import lax
from jax.experimental import pallas as pl
from jax.experimental.pallas import tpu as pltpu
from jax.sharding import PartitionSpec as P

MESH = pl.DeviceIdType.MESH
ANY = pl.BlockSpec(memory_space=pl.ANY)
VMEM_LIMIT = 60 * 2**20
C0 = 0.7978845608028654
C1 = C0 * 0.044715


def act_and_back(gate, up, d_hidden):
    g = gate.astype(jnp.float32)
    u = up.astype(jnp.float32)
    g2 = g * g
    t = jnp.tanh(g * (C0 + C1 * g2))
    cdf = 0.5 + 0.5 * t
    gelu = g * cdf
    slope = cdf + (0.5 * g) * (1.0 - t * t) * (C0 + (3.0 * C1) * g2)
    return gelu * u, d_hidden * u * slope, d_hidden * gelu


def nt(a, b):
    return lax.dot_general(a, b, (((1,), (1,)), ((), ())), preferred_element_type=jnp.float32)


def tn(a, b):
    return lax.dot_general(a, b, (((0,), (0,)), ((), ())), preferred_element_type=jnp.float32)

TILE = 256
WTILE = 512


def front_kernel(
    dy_ref, x_ref, gate_ref, up_ref, wd_ref, wg_ref, wu_ref,
    dyf_ref, xf_ref, dg_ref, du_ref, h_ref, give_ref, got_ref, keep_s_ref, keep_n_ref, send_x_ref, send_y_ref,
    dgc, duc, wbuf, send_sem, recv_sem, pair_send, pair_recv, w_sem, dy_sem, wd_sem, gu_sem, out_sem, own_sem,
):
    rows, d = dy_ref.shape
    half = rows // 2
    ff = wd_ref.shape[0]
    tiles, wtiles = ff // TILE, d // WTILE
    me = lax.axis_index("tp")
    other = me + 1 - 2 * (me % 2)
    near_y = me + 2 - 4 * ((me // 2) % 2)
    near_x = me + 4 - 8 * (me // 4)
    far = near_y + 4 - 8 * (near_y // 4)
    across = other - me

    barrier = pltpu.get_barrier_semaphore()
    for peer in (other, near_y, near_x):
        pl.semaphore_signal(barrier, inc=1, device_id={"tp": peer}, device_id_type=MESH)
    pl.semaphore_wait(barrier, 3)

    def block(owner, part=None):
        if part is None:
            return pl.ds(pl.multiple_of(owner * rows, rows), rows)
        return pl.ds(pl.multiple_of(owner * rows + part * half, half), half)

    routes = [
        (me, None, other),
        (me, 0, near_x), (me, 1, near_x), (me, 0, near_y), (me, 1, near_y),
        (near_x, 0, near_y), (near_y, 1, near_x),
        (near_x, 0, other), (near_x, 1, other), (near_y, 0, other), (near_y, 1, other),
        (far, 0, other), (far, 1, other),
    ]
    places = [block(owner, part) for owner, part, _ in routes]

    class Gather:
        def __init__(self, a, own, full):
            self.a, self.own, self.full = a, own, full

        def copy(self, number):
            _, part, peer = routes[number]
            if number < 5:
                src = self.own if part is None else self.own.at[pl.ds(part * half, half), :]
            else:
                src = self.full.at[places[number], :]
            return pltpu.make_async_remote_copy(
                src_ref=src,
                dst_ref=self.full.at[places[number], :],
                send_sem=send_sem.at[self.a, number],
                recv_sem=recv_sem.at[self.a, number],
                device_id={"tp": peer},
                device_id_type=MESH,
            )

        def send(self, *numbers):
            for number in numbers:
                self.copy(number).start()

        def arrived(self, *numbers):
            for number in numbers:
                self.copy(number).wait_recv()

        def finish(self):
            for number in range(len(routes)):
                self.copy(number).wait_send()

    dys, xs = Gather(0, dy_ref, dyf_ref), Gather(1, x_ref, xf_ref)

    def pair(p):
        return pltpu.make_async_remote_copy(
            src_ref=give_ref.at[p],
            dst_ref=got_ref.at[p],
            send_sem=pair_send.at[p],
            recv_sem=pair_recv.at[p],
            device_id={"tp": other},
            device_id_type=MESH,
        )

    pieces = [
        [(other, 0), (other, 1), (me, 0), (me, 1)],
        [(near_x + across, 0), (near_y + across, 1), (near_x, 0), (near_y, 1)],
        [(near_x + across, 1), (near_y + across, 0), (near_x, 1), (near_y, 0)],
        [(far + across, 0), (far + across, 1), (far, 0), (far, 1)],
    ]
    where = [[block(*piece) for piece in part] for part in pieces]

    def w_copies(tile, slot):
        at = pl.ds(pl.multiple_of(tile * WTILE, WTILE), WTILE)
        return [
            pltpu.make_async_copy(ref.at[at, :], wbuf.at[slot, i], w_sem.at[slot, i]) for i, ref in enumerate((wg_ref, wu_ref))
        ]

    def dx(k, last, parts, ins, outs, store, hooks, heights=None):
        def body(step, *refs):
            n = step.index[0]
            slot = lax.rem(wtiles * k + n, 2)
            for copy in w_copies(n, slot):
                copy.wait()

            def ahead():
                for copy in w_copies(lax.rem(n + 1, wtiles), 1 - slot):
                    copy.start()

            if last:
                pl.when(n < wtiles - 1)(ahead)
            else:
                ahead()
            for at, hook in hooks.items():
                pl.when(n == at)(hook)
            sums = [
                nt(dgc[p, pl.ds(first, count), :], wbuf[slot, 0]) + nt(duc[p, pl.ds(first, count), :], wbuf[slot, 1])
                for p, first, count in parts
            ]
            store(sums, refs[: len(ins)], refs[len(ins) :])

        def spec(height):
            return pl.BlockSpec((height, WTILE), lambda n: (0, n))

        pltpu.emit_pipeline(
            body,
            grid=(wtiles,),
            in_specs=[spec(rows) for _ in ins],
            out_specs=[spec(height) for height in heights or [rows] * len(outs)],
            _explicit_indices=True,
        )(*ins, *outs)

    def give(k, p, hooks={}):
        def store(sums, _, outs):
            outs[0][...] = sums[0].astype(jnp.bfloat16)

        dx(k, False, [(p, 0, rows)], [], [give_ref.at[p]], store, hooks)
        pair(p).start()

    def with_acts(dyc, wdb, gub, hc):
        def dy_load(p, i):
            if p == 0 and i >= 2:
                src = dy_ref.at[pl.ds((i - 2) * half, half), :]
            else:
                src = dyf_ref.at[where[p][i], :]
            return pltpu.make_async_copy(src, dyc.at[pl.ds(i * half, half), :], dy_sem.at[i])

        def wd_copy(j):
            at = pl.ds(pl.multiple_of(j * TILE, TILE), TILE)
            return pltpu.make_async_copy(wd_ref.at[at, :], wdb.at[at, :], wd_sem.at[j])

        def gu_copies(p):
            return [
                pltpu.make_async_copy(ref.at[where[p][i], :], gub.at[j, pl.ds(i * half, half), :], gu_sem.at[j, i])
                for j, ref in enumerate((gate_ref, up_ref))
                for i in range(4)
            ]

        def out_copies(p):
            full = ((dgc.at[p], dg_ref), (duc.at[p], du_ref), (hc, h_ref))
            return [
                pltpu.make_async_copy(src.at[pl.ds(i * half, half), :], ref.at[where[p][i], :], out_sem.at[j, i])
                for j, (src, ref) in enumerate(full)
                for i in range(4)
            ]

        def act(p):
            for i in range(4):
                dy_load(p, i).wait()
            for copy in gu_copies(p):
                copy.wait()
            if p > 0:
                for copy in out_copies(p - 1):
                    copy.wait()

            def tile(j, carry):
                if p == 0:
                    wd_copy(j).wait()
                at = pl.ds(pl.multiple_of(j * TILE, TILE), TILE)
                d_hidden = nt(dyc[...], wdb[at, :])
                h, dg, du = act_and_back(gub[0, :, at], gub[1, :, at], d_hidden)
                dgc[p, :, at] = dg.astype(jnp.bfloat16)
                duc[p, :, at] = du.astype(jnp.bfloat16)
                hc[:, at] = h.astype(jnp.bfloat16)
                return carry

            lax.fori_loop(0, tiles, tile, 0)
            for copy in out_copies(p):
                copy.start()
            if p < 3:
                for copy in gu_copies(p + 1):
                    copy.start()

        def own_x(leg):
            hold = dgc.at[3, pl.ds(0, rows), :], duc.at[3, pl.ds(0, rows), :]
            cols = pl.ds(0, ff), pl.ds(ff, ff)
            return [
                pltpu.make_async_copy(
                    *((x_ref.at[:, cols[c]], hold[c]) if leg == 0 else (hold[c], xf_ref.at[block(me), cols[c]])),
                    own_sem.at[leg, c],
                )
                for c in range(2)
            ]

        def own_dy():
            return pltpu.make_async_copy(dyc.at[pl.ds(rows, rows), :], dyf_ref.at[block(me), :], own_sem.at[2, 0])

        dys.send(0, 1, 4, 2, 3)
        dy_load(0, 2).start()
        dy_load(0, 3).start()
        wd_copy(0).start()
        for copy in gu_copies(0):
            copy.start()
        wd_copy(1).start()
        dys.arrived(0)
        dy_load(0, 0).start()
        dy_load(0, 1).start()
        for j in range(2, tiles):
            wd_copy(j).start()
        for copy in own_x(0):
            copy.start()
        for copy in w_copies(0, 0):
            copy.start()
        act(0)
        own_dy().start()
        for copy in own_x(0):
            copy.wait()
        for copy in own_x(1):
            copy.start()

        def first_halves():
            dys.arrived(1, 4)
            dys.send(5, 6, 7, 10)
            xs.send(0, 1, 4, 2, 3)

        def load(p, *numbers):
            def then():
                dys.arrived(*numbers)
                for i in range(4):
                    dy_load(p, i).start()

            return then

        def load_first():
            own_dy().wait()
            for copy in own_x(1):
                copy.wait()
            load(1, 7, 10)()

        def store_s(sums, _, outs):
            outs[0][...] = sums[0].astype(jnp.bfloat16)
            outs[1][...] = sums[1]

        dx(
            0, False, [(0, 0, rows), (0, rows, rows)], [], [give_ref.at[0], keep_s_ref], store_s,
            {wtiles - 3: first_halves, wtiles - 1: load_first},
        )
        pair(0).start()
        act(1)
        dys.arrived(2, 3)
        dys.send(8, 9)
        give(1, 1, {wtiles - 1: load(2, 8, 9)})
        act(2)

        def far_halves():
            dys.arrived(5, 6)
            dys.send(11, 12)

        give(2, 2, {wtiles - 4: far_halves, wtiles - 1: load(3, 11, 12)})
        act(3)

        def first_x_halves():
            xs.arrived(1, 4)
            xs.send(5, 6, 7, 10)

        give(3, 3, {0: first_x_halves})
        for copy in out_copies(3):
            copy.wait()

    pl.run_scoped(
        with_acts,
        pltpu.VMEM((2 * rows, d), jnp.bfloat16),
        pltpu.VMEM((ff, d), jnp.bfloat16),
        pltpu.VMEM((2, 2 * rows, ff), jnp.bfloat16),
        pltpu.VMEM((2 * rows, ff), jnp.bfloat16),
    )

    for p in (1, 2):
        pair(p).wait_recv()

    def second_halves():
        xs.arrived(2, 3)
        xs.send(8, 9)

    def store_near(sums, gots, outs):
        near0, near1 = (s + g[...].astype(jnp.float32) for s, g in zip(sums, gots))
        to_x, to_y, kept = outs
        to_x[...] = near0[:half].astype(jnp.bfloat16)
        to_y[...] = near0[half:].astype(jnp.bfloat16)
        kept[...] = near1

    dx(
        4, False, [(p, rows, rows) for p in (1, 2)], [got_ref.at[1], got_ref.at[2]],
        [send_x_ref.at[0], send_y_ref.at[0], keep_n_ref], store_near, {0: second_halves}, [half, half, rows],
    )
    pair(3).wait_recv()

    def store_far(sums, gots, outs):
        total = sums[0] + gots[0][...].astype(jnp.float32)
        outs[0][...] = total[:half].astype(jnp.bfloat16)
        outs[1][...] = total[half:].astype(jnp.bfloat16)

    dx(5, True, [(3, rows, rows)], [got_ref.at[3]], [send_x_ref.at[1], send_y_ref.at[1]], store_far, {}, [half, half])
    xs.arrived(5, 6)
    xs.send(11, 12)
    xs.arrived(0, 7, 8, 9, 10, 11, 12)
    pair(0).wait_recv()
    for p in range(4):
        pair(p).wait_send()
    dys.finish()
    xs.finish()


def front(dy, x, gate, up, wd, wg, wu):
    rows, d = dy.shape
    tokens, ff = gate.shape
    bf16, f32 = jnp.bfloat16, jnp.float32
    shapes = [
        ((tokens, d), bf16), ((tokens, d), bf16), ((tokens, ff), bf16), ((tokens, ff), bf16), ((tokens, ff), bf16),
        ((4, rows, d), bf16), ((4, rows, d), bf16), ((rows, d), f32), ((rows, d), f32),
        ((2, rows // 2, d), bf16), ((2, rows // 2, d), bf16),
    ]
    dma = pltpu.SemaphoreType.DMA
    return pl.pallas_call(
        front_kernel,
        out_shape=[jax.ShapeDtypeStruct(*s) for s in shapes],
        in_specs=[ANY] * 7,
        out_specs=[ANY] * len(shapes),
        scratch_shapes=[
            pltpu.VMEM((4, 2 * rows, ff), bf16),
            pltpu.VMEM((4, 2 * rows, ff), bf16),
            pltpu.VMEM((2, 2, WTILE, ff), bf16),
            dma((2, 13)), dma((2, 13)), dma((4,)), dma((4,)), dma((2, 2)),
            dma((4,)), dma((7,)), dma((2, 4)), dma((3, 4)), dma((3, 2)),
        ],
        compiler_params=pltpu.CompilerParams(
            collective_id=0, has_side_effects=True, vmem_limit_bytes=VMEM_LIMIT
        ),
        cost_estimate=pl.CostEstimate(
            flops=6 * tokens * d * ff, bytes_accessed=300 * 2**20, transcendentals=tokens * ff
        ),
        name="front",
    )(dy, x, gate, up, wd, wg, wu)


def dw_kernel(a_ref, b_ref, o_ref):
    o_ref[...] = tn(a_ref[...], b_ref[...]).astype(o_ref.dtype)


def dw(a, b, tm=512):
    tokens, m = a.shape
    n = b.shape[1]
    return pl.pallas_call(
        dw_kernel,
        out_shape=jax.ShapeDtypeStruct((m, n), jnp.bfloat16),
        grid=(m // tm,),
        in_specs=[
            pl.BlockSpec((tokens, tm), lambda i: (0, i)),
            pl.BlockSpec((tokens, n), lambda i: (0, 0), pipeline_mode=pl.Buffered(1)),
        ],
        out_specs=pl.BlockSpec((tm, n), lambda i: (i, 0)),
        compiler_params=pltpu.CompilerParams(dimension_semantics=("arbitrary",), vmem_limit_bytes=VMEM_LIMIT),
        cost_estimate=pl.CostEstimate(
            flops=2 * tokens * m * n, bytes_accessed=2 * (tokens * m + tokens * n + m * n), transcendentals=0
        ),
        name="dw",
    )(a, b)


def dw_two(h, dy, x, dg, tile=512):
    tokens, ff = h.shape
    d = dy.shape[1]
    steps = d // tile

    def kernel(h_ref, dy_ref, x_ref, dg_hbm, down_ref, gate_ref, held, sem):
        i = pl.program_id(0)
        load = pltpu.make_async_copy(dg_hbm, held, sem)

        @pl.when(i == 0)
        def _():
            load.start()

        @pl.when(i < steps)
        def _():
            down_ref[...] = tn(h_ref[...], dy_ref[...]).astype(down_ref.dtype)

        @pl.when(i == steps - 1)
        def _():
            load.wait()

        @pl.when(i >= steps)
        def _():
            gate_ref[...] = tn(x_ref[...], held[...]).astype(gate_ref.dtype)

    def first(i):
        return jnp.minimum(i, steps - 1)

    def second(i):
        return jnp.maximum(i - steps, 0)

    return pl.pallas_call(
        kernel,
        out_shape=[jax.ShapeDtypeStruct((ff, d), jnp.bfloat16), jax.ShapeDtypeStruct((d, ff), jnp.bfloat16)],
        grid=(2 * steps,),
        in_specs=[
            pl.BlockSpec((tokens, ff), lambda i: (0, 0), pipeline_mode=pl.Buffered(1)),
            pl.BlockSpec((tokens, tile), lambda i: (0, first(i))),
            pl.BlockSpec((tokens, tile), lambda i: (0, second(i))),
            ANY,
        ],
        out_specs=[
            pl.BlockSpec((ff, tile), lambda i: (0, first(i))),
            pl.BlockSpec((tile, ff), lambda i: (second(i), 0)),
        ],
        scratch_shapes=[pltpu.VMEM((tokens, ff), jnp.bfloat16), pltpu.SemaphoreType.DMA(())],
        compiler_params=pltpu.CompilerParams(dimension_semantics=("arbitrary",), vmem_limit_bytes=VMEM_LIMIT),
        cost_estimate=pl.CostEstimate(
            flops=4 * tokens * d * ff, bytes_accessed=4 * (tokens * d + tokens * ff + d * ff), transcendentals=0
        ),
        name="dw_two",
    )(h, dy, x, dg)


def sum_on(kept, from_x, from_y, tile=1792):
    rows, d = kept.shape
    half = rows // 2

    def kernel(kept_ref, fx_ref, fy_ref, ony_ref, onx_ref):
        onx_ref[...] = (kept_ref[pl.ds(0, half), :] + fy_ref[0].astype(jnp.float32)).astype(jnp.bfloat16)
        ony_ref[...] = (kept_ref[pl.ds(half, half), :] + fx_ref[0].astype(jnp.float32)).astype(jnp.bfloat16)

    part = pl.BlockSpec((1, half, tile), lambda i: (1, 0, i))
    out = pl.BlockSpec((half, tile), lambda i: (0, i))
    return pl.pallas_call(
        kernel,
        out_shape=[jax.ShapeDtypeStruct((half, d), jnp.bfloat16)] * 2,
        grid=(d // tile,),
        in_specs=[pl.BlockSpec((rows, tile), lambda i: (0, i)), part, part],
        out_specs=[out, out],
        compiler_params=pltpu.CompilerParams(dimension_semantics=("arbitrary",), vmem_limit_bytes=VMEM_LIMIT),
        cost_estimate=pl.CostEstimate(flops=rows * d, bytes_accessed=8 * rows * d, transcendentals=0),
        name="sum_on",
    )(kept, from_x, from_y)


def sum_rows(kept, got, from_x, from_y, last_x, last_y, tile=896):
    rows, d = kept.shape
    half = rows // 2

    def kernel(kept_ref, got_ref, fx_ref, fy_ref, lx_ref, ly_ref, o_ref):
        f32 = jnp.float32
        for at, near, last in ((pl.ds(0, half), fx_ref, ly_ref), (pl.ds(half, half), fy_ref, lx_ref)):
            total = kept_ref[at, :] + got_ref[0, at, :].astype(f32) + near[0].astype(f32) + last[...].astype(f32)
            o_ref[at, :] = total.astype(o_ref.dtype)

    full = pl.BlockSpec((rows, tile), lambda i: (0, i))
    part = pl.BlockSpec((1, half, tile), lambda i: (0, 0, i))
    last = pl.BlockSpec((half, tile), lambda i: (0, i))
    return pl.pallas_call(
        kernel,
        out_shape=jax.ShapeDtypeStruct((rows, d), jnp.bfloat16),
        grid=(d // tile,),
        in_specs=[full, pl.BlockSpec((1, rows, tile), lambda i: (0, 0, i)), part, part, last, last],
        out_specs=full,
        compiler_params=pltpu.CompilerParams(dimension_semantics=("arbitrary",), vmem_limit_bytes=VMEM_LIMIT),
        cost_estimate=pl.CostEstimate(flops=4 * rows * d, bytes_accessed=14 * rows * d, transcendentals=0),
        name="sum_rows",
    )(kept, got, from_x, from_y, last_x, last_y)


def solution(mesh):
    devices = mesh.shape["tp"]
    to_x = [(i, i ^ 4) for i in range(devices)]
    to_y = [(i, i ^ 2) for i in range(devices)]

    def step(x, dy, gate, up, wg, wu, wd):
        dyf, xf, dg, du, h, _, got, keep_s, keep_n, send_x, send_y = front(dy, x, gate, up, wd, wg, wu)
        from_x = lax.ppermute(send_x, "tp", to_x)
        from_y = lax.ppermute(send_y, "tp", to_y)
        dw_down, dw_gate = dw_two(h, dyf, xf, dg)
        on_y, on_x = sum_on(keep_n, from_x, from_y)
        du, on_y, on_x = lax.optimization_barrier((du, on_y, on_x))
        last_y = lax.ppermute(on_y, "tp", to_y)
        last_x = lax.ppermute(on_x, "tp", to_x)
        dw_up = dw(xf, du)
        dx = sum_rows(keep_s, got, from_x, from_y, last_x, last_y)
        return dx, dw_gate, dw_up, dw_down

    rows, cols, down = P(("dp", "tp"), None), P("dp", "tp"), P("tp", None)
    weight = P(None, "tp")
    return jax.shard_map(
        step,
        mesh=mesh,
        in_specs=(rows, rows, cols, cols, weight, weight, down),
        out_specs=(rows, cols, cols, P(("dp", "tp"), None)),
        check_vma=False,
    )
```

```python
import jax
import jax.numpy as jnp
from jax import lax
from jax.experimental import pallas as pl
from jax.experimental.pallas import tpu as pltpu
from jax.sharding import PartitionSpec as P

MESH = pl.DeviceIdType.MESH
ANY = pl.BlockSpec(memory_space=pl.ANY)
VMEM_LIMIT = 67043328
C0 = 0.7978845608028654
C1 = C0 * 0.044715


def act_and_back(gate, up, d_hidden):
    g = gate.astype(jnp.float32)
    u = up.astype(jnp.float32)
    g2 = g * g
    t = jnp.tanh(g * (C0 + C1 * g2))
    cdf = 0.5 + 0.5 * t
    gelu = g * cdf
    slope = cdf + (0.5 * g) * (1.0 - t * t) * (C0 + (3.0 * C1) * g2)
    return gelu * u, d_hidden * u * slope, d_hidden * gelu


def nt(a, b):
    return lax.dot_general(a, b, (((1,), (1,)), ((), ())), preferred_element_type=jnp.float32)


def tn(a, b):
    return lax.dot_general(a, b, (((0,), (0,)), ((), ())), preferred_element_type=jnp.float32)

TILE = 256
WTILE = 512


def front_kernel(
    dy_ref, x_ref, gate_ref, up_ref, wd_ref, wg_ref, wu_ref,
    dyf_ref, xf_ref, dg_ref, du_ref, h_ref, give_ref, got_ref, keep_s_ref, keep_n_ref, send_x_ref, send_y_ref,
    dgc, duc, wbuf, send_sem, recv_sem, pair_send, pair_recv, w_sem, dy_sem, wd_sem, gu_sem, out_sem, own_sem,
):
    rows, d = dy_ref.shape
    half = rows // 2
    ff = wd_ref.shape[0]
    tiles, wtiles = ff // TILE, d // WTILE
    me = lax.axis_index("tp")
    other = me + 1 - 2 * (me % 2)
    near_y = me + 2 - 4 * ((me // 2) % 2)
    near_x = me + 4 - 8 * (me // 4)
    far = near_y + 4 - 8 * (near_y // 4)
    across = other - me

    barrier = pltpu.get_barrier_semaphore()
    for peer in (other, near_y, near_x):
        pl.semaphore_signal(barrier, inc=1, device_id={"tp": peer}, device_id_type=MESH)
    pl.semaphore_wait(barrier, 3)

    def block(owner, part=None):
        if part is None:
            return pl.ds(pl.multiple_of(owner * rows, rows), rows)
        return pl.ds(pl.multiple_of(owner * rows + part * half, half), half)

    routes = [
        (me, None, other),
        (me, 0, near_x), (me, 1, near_x), (me, 0, near_y), (me, 1, near_y),
        (near_x, 0, near_y), (near_y, 1, near_x),
        (near_x, 0, other), (near_x, 1, other), (near_y, 0, other), (near_y, 1, other),
        (far, 0, other), (far, 1, other),
    ]
    places = [block(owner, part) for owner, part, _ in routes]

    class Gather:
        def __init__(self, a, own, full):
            self.a, self.own, self.full = a, own, full

        def copy(self, number):
            _, part, peer = routes[number]
            if number < 5:
                src = self.own if part is None else self.own.at[pl.ds(part * half, half), :]
            else:
                src = self.full.at[places[number], :]
            return pltpu.make_async_remote_copy(
                src_ref=src,
                dst_ref=self.full.at[places[number], :],
                send_sem=send_sem.at[self.a, number],
                recv_sem=recv_sem.at[self.a, number],
                device_id={"tp": peer},
                device_id_type=MESH,
            )

        def send(self, *numbers):
            for number in numbers:
                self.copy(number).start()

        def arrived(self, *numbers):
            for number in numbers:
                self.copy(number).wait_recv()

        def finish(self):
            for number in range(len(routes)):
                self.copy(number).wait_send()

    dys, xs = Gather(0, dy_ref, dyf_ref), Gather(1, x_ref, xf_ref)

    def pair(p):
        return pltpu.make_async_remote_copy(
            src_ref=give_ref.at[p],
            dst_ref=got_ref.at[p],
            send_sem=pair_send.at[p],
            recv_sem=pair_recv.at[p],
            device_id={"tp": other},
            device_id_type=MESH,
        )

    pieces = [
        [(other, 0), (other, 1), (me, 0), (me, 1)],
        [(near_x + across, 0), (near_y + across, 1), (near_x, 0), (near_y, 1)],
        [(near_x + across, 1), (near_y + across, 0), (near_x, 1), (near_y, 0)],
        [(far + across, 0), (far + across, 1), (far, 0), (far, 1)],
    ]
    where = [[block(*piece) for piece in part] for part in pieces]

    def w_rows(tile):
        return pl.ds(pl.multiple_of(tile * WTILE, WTILE), WTILE)

    def w_copies(tile):
        at = w_rows(tile)
        return [
            pltpu.make_async_copy(ref.at[at, :], wbuf.at[i, at, :], w_sem.at[tile, i]) for i, ref in enumerate((wg_ref, wu_ref))
        ]

    def dx(first_pass, parts, ins, outs, store, hooks, heights=None):
        def body(step, *refs):
            n = step.index[0]
            at = w_rows(n)
            if first_pass:
                for copy in w_copies(n):
                    copy.wait()

                @pl.when(n + 3 < wtiles)
                def _():
                    for copy in w_copies(n + 3):
                        copy.start()

            for when, hook in hooks.items():
                pl.when(n == when)(hook)
            sums = [
                nt(dgc[p, pl.ds(first, count), :], wbuf[0, at, :]) + nt(duc[p, pl.ds(first, count), :], wbuf[1, at, :])
                for p, first, count in parts
            ]
            store(sums, refs[: len(ins)], refs[len(ins) :])

        def spec(height):
            return pl.BlockSpec((height, WTILE), lambda n: (0, n))

        pltpu.emit_pipeline(
            body,
            grid=(wtiles,),
            in_specs=[spec(rows) for _ in ins],
            out_specs=[spec(height) for height in heights or [rows] * len(outs)],
            _explicit_indices=True,
        )(*ins, *outs)

    def give(p, hooks={}):
        def store(sums, _, outs):
            outs[0][...] = sums[0].astype(jnp.bfloat16)

        dx(False, [(p, 0, rows)], [], [give_ref.at[p]], store, hooks)
        pair(p).start()

    def with_acts(dyc, wdb, gub, hc):
        def dy_load(p, i):
            if p == 0 and i >= 2:
                src = dy_ref.at[pl.ds((i - 2) * half, half), :]
            else:
                src = dyf_ref.at[where[p][i], :]
            return pltpu.make_async_copy(src, dyc.at[pl.ds(i * half, half), :], dy_sem.at[i])

        def wd_copy(j, slot):
            at = pl.ds(pl.multiple_of(j * TILE, TILE), TILE)
            return pltpu.make_async_copy(wd_ref.at[at, :], wdb.at[slot], wd_sem.at[slot])

        def gu_copies(p):
            return [
                pltpu.make_async_copy(ref.at[where[p][i], :], gub.at[j, pl.ds(i * half, half), :], gu_sem.at[j, i])
                for j, ref in enumerate((gate_ref, up_ref))
                for i in range(4)
            ]

        def out_copies(p):
            full = ((dgc.at[p], dg_ref), (duc.at[p], du_ref), (hc, h_ref))
            return [
                pltpu.make_async_copy(src.at[pl.ds(i * half, half), :], ref.at[where[p][i], :], out_sem.at[j, i])
                for j, (src, ref) in enumerate(full)
                for i in range(4)
            ]

        def act(p):
            for i in range(4):
                dy_load(p, i).wait()
            for copy in gu_copies(p):
                copy.wait()
            if p > 0:
                for copy in out_copies(p - 1):
                    copy.wait()

            def tile(j, carry):
                count = tiles * p + j
                slot = lax.rem(count, 2)
                wd_copy(j, slot).wait()

                def ahead():
                    wd_copy(lax.rem(j + 1, tiles), 1 - slot).start()

                if p < 3:
                    ahead()
                else:
                    pl.when(j < tiles - 1)(ahead)
                if p == 0:

                    @pl.when((j > 0) & (j < 4))
                    def _():
                        for copy in w_copies(j - 1):
                            copy.start()

                at = pl.ds(pl.multiple_of(j * TILE, TILE), TILE)
                d_hidden = nt(dyc[...], wdb[slot])
                h, dg, du = act_and_back(gub[0, :, at], gub[1, :, at], d_hidden)
                dgc[p, :, at] = dg.astype(jnp.bfloat16)
                duc[p, :, at] = du.astype(jnp.bfloat16)
                hc[:, at] = h.astype(jnp.bfloat16)
                return carry

            lax.fori_loop(0, tiles, tile, 0)
            for copy in out_copies(p):
                copy.start()
            if p < 3:
                for copy in gu_copies(p + 1):
                    copy.start()

        def own_x(leg):
            hold = dgc.at[3, pl.ds(0, rows), :], duc.at[3, pl.ds(0, rows), :]
            cols = pl.ds(0, ff), pl.ds(ff, ff)
            return [
                pltpu.make_async_copy(
                    *((x_ref.at[:, cols[c]], hold[c]) if leg == 0 else (hold[c], xf_ref.at[block(me), cols[c]])),
                    own_sem.at[leg, c],
                )
                for c in range(2)
            ]

        def own_dy():
            return pltpu.make_async_copy(dyc.at[pl.ds(rows, rows), :], dyf_ref.at[block(me), :], own_sem.at[2, 0])

        dys.send(0, 1, 4, 2, 3)
        dy_load(0, 2).start()
        dy_load(0, 3).start()
        wd_copy(0, 0).start()
        for copy in gu_copies(0):
            copy.start()
        dys.arrived(0)
        dy_load(0, 0).start()
        dy_load(0, 1).start()
        for copy in own_x(0):
            copy.start()
        act(0)
        own_dy().start()
        for copy in own_x(0):
            copy.wait()
        for copy in own_x(1):
            copy.start()

        def first_halves():
            dys.arrived(1, 4)
            dys.send(5, 6, 7, 10)
            xs.send(0, 1, 4, 2, 3)

        def load(p, *numbers):
            def then():
                dys.arrived(*numbers)
                for i in range(4):
                    dy_load(p, i).start()

            return then

        def load_first():
            own_dy().wait()
            for copy in own_x(1):
                copy.wait()
            load(1, 7, 10)()

        def store_s(sums, _, outs):
            outs[0][...] = sums[0].astype(jnp.bfloat16)
            outs[1][...] = sums[1]

        dx(
            True, [(0, 0, rows), (0, rows, rows)], [], [give_ref.at[0], keep_s_ref], store_s,
            {wtiles - 3: first_halves, wtiles - 1: load_first},
        )
        pair(0).start()
        act(1)
        dys.arrived(2, 3)
        dys.send(8, 9)
        give(1, {wtiles - 1: load(2, 8, 9)})
        act(2)

        def far_halves():
            dys.arrived(5, 6)
            dys.send(11, 12)

        give(2, {wtiles - 4: far_halves, wtiles - 1: load(3, 11, 12)})
        act(3)

        def first_x_halves():
            xs.arrived(1, 4)
            xs.send(5, 6, 7, 10)

        give(3, {0: first_x_halves})
        for copy in out_copies(3):
            copy.wait()

    pl.run_scoped(
        with_acts,
        pltpu.VMEM((2 * rows, d), jnp.bfloat16),
        pltpu.VMEM((2, TILE, d), jnp.bfloat16),
        pltpu.VMEM((2, 2 * rows, ff), jnp.bfloat16),
        pltpu.VMEM((2 * rows, ff), jnp.bfloat16),
    )

    for p in (1, 2):
        pair(p).wait_recv()

    def second_halves():
        xs.arrived(2, 3)
        xs.send(8, 9)

    def store_near(sums, gots, outs):
        near0, near1 = (s + g[...].astype(jnp.float32) for s, g in zip(sums, gots))
        to_x, to_y, kept = outs
        to_x[...] = near0[:half].astype(jnp.bfloat16)
        to_y[...] = near0[half:].astype(jnp.bfloat16)
        kept[...] = near1

    dx(
        False, [(p, rows, rows) for p in (1, 2)], [got_ref.at[1], got_ref.at[2]],
        [send_x_ref.at[0], send_y_ref.at[0], keep_n_ref], store_near, {0: second_halves}, [half, half, rows],
    )
    pair(3).wait_recv()

    def store_far(sums, gots, outs):
        total = sums[0] + gots[0][...].astype(jnp.float32)
        outs[0][...] = total[:half].astype(jnp.bfloat16)
        outs[1][...] = total[half:].astype(jnp.bfloat16)

    dx(False, [(3, rows, rows)], [got_ref.at[3]], [send_x_ref.at[1], send_y_ref.at[1]], store_far, {}, [half, half])
    xs.arrived(5, 6)
    xs.send(11, 12)
    xs.arrived(0, 7, 8, 9, 10, 11, 12)
    pair(0).wait_recv()
    for p in range(4):
        pair(p).wait_send()
    dys.finish()
    xs.finish()


def front(dy, x, gate, up, wd, wg, wu):
    rows, d = dy.shape
    tokens, ff = gate.shape
    bf16, f32 = jnp.bfloat16, jnp.float32
    shapes = [
        ((tokens, d), bf16), ((tokens, d), bf16), ((tokens, ff), bf16), ((tokens, ff), bf16), ((tokens, ff), bf16),
        ((4, rows, d), bf16), ((4, rows, d), bf16), ((rows, d), f32), ((rows, d), f32),
        ((2, rows // 2, d), bf16), ((2, rows // 2, d), bf16),
    ]
    dma = pltpu.SemaphoreType.DMA
    return pl.pallas_call(
        front_kernel,
        out_shape=[jax.ShapeDtypeStruct(*s) for s in shapes],
        in_specs=[ANY] * 7,
        out_specs=[ANY] * len(shapes),
        scratch_shapes=[
            pltpu.VMEM((4, 2 * rows, ff), bf16),
            pltpu.VMEM((4, 2 * rows, ff), bf16),
            pltpu.VMEM((2, d, ff), bf16),
            dma((2, 13)), dma((2, 13)), dma((4,)), dma((4,)), dma((d // WTILE, 2)),
            dma((4,)), dma((2,)), dma((2, 4)), dma((3, 4)), dma((3, 2)),
        ],
        compiler_params=pltpu.CompilerParams(
            collective_id=0, has_side_effects=True, vmem_limit_bytes=VMEM_LIMIT
        ),
        cost_estimate=pl.CostEstimate(
            flops=6 * tokens * d * ff, bytes_accessed=300 * 2**20, transcendentals=tokens * ff
        ),
        name="front",
    )(dy, x, gate, up, wd, wg, wu)


def dw_kernel(a_ref, b_ref, o_ref):
    o_ref[...] = tn(a_ref[...], b_ref[...]).astype(o_ref.dtype)


def dw(a, b, tm=512):
    tokens, m = a.shape
    n = b.shape[1]
    return pl.pallas_call(
        dw_kernel,
        out_shape=jax.ShapeDtypeStruct((m, n), jnp.bfloat16),
        grid=(m // tm,),
        in_specs=[
            pl.BlockSpec((tokens, tm), lambda i: (0, i)),
            pl.BlockSpec((tokens, n), lambda i: (0, 0), pipeline_mode=pl.Buffered(1)),
        ],
        out_specs=pl.BlockSpec((tm, n), lambda i: (i, 0)),
        compiler_params=pltpu.CompilerParams(dimension_semantics=("arbitrary",), vmem_limit_bytes=VMEM_LIMIT),
        cost_estimate=pl.CostEstimate(
            flops=2 * tokens * m * n, bytes_accessed=2 * (tokens * m + tokens * n + m * n), transcendentals=0
        ),
        name="dw",
    )(a, b)


def dw_two(h, dy, x, dg, tile=512):
    tokens, ff = h.shape
    d = dy.shape[1]
    steps = d // tile

    def kernel(h_ref, dy_ref, x_ref, dg_hbm, down_ref, gate_ref, held, sem):
        i = pl.program_id(0)
        load = pltpu.make_async_copy(dg_hbm, held, sem)

        @pl.when(i == 0)
        def _():
            load.start()

        @pl.when(i < steps)
        def _():
            down_ref[...] = tn(h_ref[...], dy_ref[...]).astype(down_ref.dtype)

        @pl.when(i == steps - 1)
        def _():
            load.wait()

        @pl.when(i >= steps)
        def _():
            gate_ref[...] = tn(x_ref[...], held[...]).astype(gate_ref.dtype)

    def first(i):
        return jnp.minimum(i, steps - 1)

    def second(i):
        return jnp.maximum(i - steps, 0)

    return pl.pallas_call(
        kernel,
        out_shape=[jax.ShapeDtypeStruct((ff, d), jnp.bfloat16), jax.ShapeDtypeStruct((d, ff), jnp.bfloat16)],
        grid=(2 * steps,),
        in_specs=[
            pl.BlockSpec((tokens, ff), lambda i: (0, 0), pipeline_mode=pl.Buffered(1)),
            pl.BlockSpec((tokens, tile), lambda i: (0, first(i))),
            pl.BlockSpec((tokens, tile), lambda i: (0, second(i))),
            ANY,
        ],
        out_specs=[
            pl.BlockSpec((ff, tile), lambda i: (0, first(i))),
            pl.BlockSpec((tile, ff), lambda i: (second(i), 0)),
        ],
        scratch_shapes=[pltpu.VMEM((tokens, ff), jnp.bfloat16), pltpu.SemaphoreType.DMA(())],
        compiler_params=pltpu.CompilerParams(dimension_semantics=("arbitrary",), vmem_limit_bytes=VMEM_LIMIT),
        cost_estimate=pl.CostEstimate(
            flops=4 * tokens * d * ff, bytes_accessed=4 * (tokens * d + tokens * ff + d * ff), transcendentals=0
        ),
        name="dw_two",
    )(h, dy, x, dg)


def sum_on(kept, from_x, from_y, tile=1792):
    rows, d = kept.shape
    half = rows // 2

    def kernel(kept_ref, fx_ref, fy_ref, ony_ref, onx_ref):
        onx_ref[...] = (kept_ref[pl.ds(0, half), :] + fy_ref[0].astype(jnp.float32)).astype(jnp.bfloat16)
        ony_ref[...] = (kept_ref[pl.ds(half, half), :] + fx_ref[0].astype(jnp.float32)).astype(jnp.bfloat16)

    part = pl.BlockSpec((1, half, tile), lambda i: (1, 0, i))
    out = pl.BlockSpec((half, tile), lambda i: (0, i))
    return pl.pallas_call(
        kernel,
        out_shape=[jax.ShapeDtypeStruct((half, d), jnp.bfloat16)] * 2,
        grid=(d // tile,),
        in_specs=[pl.BlockSpec((rows, tile), lambda i: (0, i)), part, part],
        out_specs=[out, out],
        compiler_params=pltpu.CompilerParams(dimension_semantics=("arbitrary",), vmem_limit_bytes=VMEM_LIMIT),
        cost_estimate=pl.CostEstimate(flops=rows * d, bytes_accessed=8 * rows * d, transcendentals=0),
        name="sum_on",
    )(kept, from_x, from_y)


def sum_rows(kept, got, from_x, from_y, last_x, last_y, tile=896):
    rows, d = kept.shape
    half = rows // 2

    def kernel(kept_ref, got_ref, fx_ref, fy_ref, lx_ref, ly_ref, o_ref):
        f32 = jnp.float32
        for at, near, last in ((pl.ds(0, half), fx_ref, ly_ref), (pl.ds(half, half), fy_ref, lx_ref)):
            total = kept_ref[at, :] + got_ref[0, at, :].astype(f32) + near[0].astype(f32) + last[...].astype(f32)
            o_ref[at, :] = total.astype(o_ref.dtype)

    full = pl.BlockSpec((rows, tile), lambda i: (0, i))
    part = pl.BlockSpec((1, half, tile), lambda i: (0, 0, i))
    last = pl.BlockSpec((half, tile), lambda i: (0, i))
    return pl.pallas_call(
        kernel,
        out_shape=jax.ShapeDtypeStruct((rows, d), jnp.bfloat16),
        grid=(d // tile,),
        in_specs=[full, pl.BlockSpec((1, rows, tile), lambda i: (0, 0, i)), part, part, last, last],
        out_specs=full,
        compiler_params=pltpu.CompilerParams(dimension_semantics=("arbitrary",), vmem_limit_bytes=VMEM_LIMIT),
        cost_estimate=pl.CostEstimate(flops=4 * rows * d, bytes_accessed=14 * rows * d, transcendentals=0),
        name="sum_rows",
    )(kept, got, from_x, from_y, last_x, last_y)


def solution(mesh):
    devices = mesh.shape["tp"]
    to_x = [(i, i ^ 4) for i in range(devices)]
    to_y = [(i, i ^ 2) for i in range(devices)]

    def step(x, dy, gate, up, wg, wu, wd):
        dyf, xf, dg, du, h, _, got, keep_s, keep_n, send_x, send_y = front(dy, x, gate, up, wd, wg, wu)
        from_x = lax.ppermute(send_x, "tp", to_x)
        from_y = lax.ppermute(send_y, "tp", to_y)
        dw_down, dw_gate = dw_two(h, dyf, xf, dg)
        on_y, on_x = sum_on(keep_n, from_x, from_y)
        du, on_y, on_x = lax.optimization_barrier((du, on_y, on_x))
        last_y = lax.ppermute(on_y, "tp", to_y)
        last_x = lax.ppermute(on_x, "tp", to_x)
        dw_up = dw(xf, du)
        dx = sum_rows(keep_s, got, from_x, from_y, last_x, last_y)
        return dx, dw_gate, dw_up, dw_down

    rows, cols, down = P(("dp", "tp"), None), P("dp", "tp"), P("tp", None)
    weight = P(None, "tp")
    return jax.shard_map(
        step,
        mesh=mesh,
        in_specs=(rows, rows, cols, cols, weight, weight, down),
        out_specs=(rows, cols, cols, P(("dp", "tp"), None)),
        check_vma=False,
    )
```

```python
import jax
import jax.numpy as jnp
from jax import lax
from jax.experimental import pallas as pl
from jax.experimental.pallas import tpu as pltpu
from jax.sharding import PartitionSpec as P

MESH = pl.DeviceIdType.MESH
ANY = pl.BlockSpec(memory_space=pl.ANY)
VMEM_LIMIT = 67043328
C0 = 0.7978845608028654
C1 = C0 * 0.044715


def act_and_back(gate, up, d_hidden):
    g = gate.astype(jnp.float32)
    u = up.astype(jnp.float32)
    g2 = g * g
    t = jnp.tanh(g * (C0 + C1 * g2))
    cdf = 0.5 + 0.5 * t
    gelu = g * cdf
    slope = cdf + (0.5 * g) * (1.0 - t * t) * (C0 + (3.0 * C1) * g2)
    return gelu * u, d_hidden * u * slope, d_hidden * gelu


def nt(a, b):
    return lax.dot_general(a, b, (((1,), (1,)), ((), ())), preferred_element_type=jnp.float32)


def tn(a, b):
    return lax.dot_general(a, b, (((0,), (0,)), ((), ())), preferred_element_type=jnp.float32)

TILE = 256
WTILE = 512


def front_kernel(
    dy_ref, x_ref, gate_ref, up_ref, wd_ref, wg_ref, wu_ref,
    dyf_ref, xf_ref, dg_ref, du_ref, h_ref, give_ref, got_s_ref, got_ref, keep_s_ref, keep_n_ref, send_x_ref, send_y_ref,
    dgc, duc, wbuf, send_sem, recv_sem, pair_send, pair_recv, w_sem, dy_sem, wd_sem, gu_sem, out_sem, own_sem,
):
    rows, d = dy_ref.shape
    half = rows // 2
    ff = wd_ref.shape[0]
    tiles, wtiles = ff // TILE, d // WTILE
    me = lax.axis_index("tp")
    other = me + 1 - 2 * (me % 2)
    near_y = me + 2 - 4 * ((me // 2) % 2)
    near_x = me + 4 - 8 * (me // 4)
    far = near_y + 4 - 8 * (near_y // 4)
    across = other - me

    barrier = pltpu.get_barrier_semaphore()
    for peer in (other, near_y, near_x):
        pl.semaphore_signal(barrier, inc=1, device_id={"tp": peer}, device_id_type=MESH)
    pl.semaphore_wait(barrier, 3)

    quarter = half // 2

    def block(owner, start=0, count=rows):
        return pl.ds(pl.multiple_of(owner * rows + start, count), count)

    routes = [
        (me, 0, rows, other),
        (me, 0, half, near_x), (me, half, half, near_x), (me, 0, half, near_y), (me, half, half, near_y),
        (near_x, 0, quarter, near_y), (near_y, half, quarter, near_x),
        (near_x, 0, half, other), (near_x, half, half, other), (near_y, 0, half, other), (near_y, half, half, other),
        (far, 0, quarter, other), (far, half, quarter, other),
        (near_x, quarter, quarter, near_y), (near_y, half + quarter, quarter, near_x),
        (far, quarter, quarter, other), (far, half + quarter, quarter, other),
    ]
    places = [block(owner, start, count) for owner, start, count, _ in routes]

    class Gather:
        def __init__(self, a, own, full):
            self.a, self.own, self.full = a, own, full

        def copy(self, number):
            _, start, count, peer = routes[number]
            if number < 5:
                src = self.own.at[pl.ds(start, count), :]
            else:
                src = self.full.at[places[number], :]
            return pltpu.make_async_remote_copy(
                src_ref=src,
                dst_ref=self.full.at[places[number], :],
                send_sem=send_sem.at[self.a, number],
                recv_sem=recv_sem.at[self.a, number],
                device_id={"tp": peer},
                device_id_type=MESH,
            )

        def send(self, *numbers):
            for number in numbers:
                self.copy(number).start()

        def arrived(self, *numbers):
            for number in numbers:
                self.copy(number).wait_recv()

        def finish(self):
            for number in range(len(routes)):
                self.copy(number).wait_send()

    dys, xs = Gather(0, dy_ref, dyf_ref), Gather(1, x_ref, xf_ref)

    def pair(p):
        return pltpu.make_async_remote_copy(
            src_ref=give_ref.at[p],
            dst_ref=got_s_ref if p == 0 else got_ref.at[p - 1],
            send_sem=pair_send.at[p],
            recv_sem=pair_recv.at[p],
            device_id={"tp": other},
            device_id_type=MESH,
        )

    pieces = [
        [(other, 0), (other, 1), (me, 0), (me, 1)],
        [(near_x + across, 0), (near_y + across, 1), (near_x, 0), (near_y, 1)],
        [(near_x + across, 1), (near_y + across, 0), (near_x, 1), (near_y, 0)],
        [(far + across, 0), (far + across, 1), (far, 0), (far, 1)],
    ]
    where = [[block(owner, part * half, half) for owner, part in some] for some in pieces]

    def w_rows(tile):
        return pl.ds(pl.multiple_of(tile * WTILE, WTILE), WTILE)

    def w_copies(tile):
        at = w_rows(tile)
        return [
            pltpu.make_async_copy(ref.at[at, :], wbuf.at[i, at, :], w_sem.at[tile, i]) for i, ref in enumerate((wg_ref, wu_ref))
        ]

    def dx(first_pass, parts, ins, outs, store, hooks, heights=None):
        def body(step, *refs):
            n = step.index[0]
            at = w_rows(n)
            if first_pass:
                for copy in w_copies(n):
                    copy.wait()

                @pl.when(n + 3 < wtiles)
                def _():
                    for copy in w_copies(n + 3):
                        copy.start()

            for when, hook in hooks.items():
                pl.when(n == when)(hook)
            sums = [
                nt(dgc[p, pl.ds(first, count), :], wbuf[0, at, :]) + nt(duc[p, pl.ds(first, count), :], wbuf[1, at, :])
                for p, first, count in parts
            ]
            store(sums, refs[: len(ins)], refs[len(ins) :])

        def spec(height):
            return pl.BlockSpec((height, WTILE), lambda n: (0, n))

        pltpu.emit_pipeline(
            body,
            grid=(wtiles,),
            in_specs=[spec(rows) for _ in ins],
            out_specs=[spec(height) for height in heights or [rows] * len(outs)],
            _explicit_indices=True,
        )(*ins, *outs)

    def give(p, hooks={}):
        def store(sums, _, outs):
            outs[0][...] = sums[0].astype(jnp.bfloat16)

        dx(False, [(p, 0, rows)], [], [give_ref.at[p]], store, hooks)
        pair(p).start()

    def with_acts(dyc, wdb, gub, hc):
        def dy_load(p, i):
            if p == 0 and i >= 2:
                src = dy_ref.at[pl.ds((i - 2) * half, half), :]
            else:
                src = dyf_ref.at[where[p][i], :]
            return pltpu.make_async_copy(src, dyc.at[pl.ds(i * half, half), :], dy_sem.at[i])

        def wd_copy(j, slot):
            at = pl.ds(pl.multiple_of(j * TILE, TILE), TILE)
            return pltpu.make_async_copy(wd_ref.at[at, :], wdb.at[slot], wd_sem.at[slot])

        def gu_copies(p):
            return [
                pltpu.make_async_copy(ref.at[where[p][i], :], gub.at[j, pl.ds(i * half, half), :], gu_sem.at[j, i])
                for j, ref in enumerate((gate_ref, up_ref))
                for i in range(4)
            ]

        def out_copies(p):
            full = ((dgc.at[p], dg_ref), (duc.at[p], du_ref), (hc, h_ref))
            return [
                pltpu.make_async_copy(src.at[pl.ds(i * half, half), :], ref.at[where[p][i], :], out_sem.at[j, i])
                for j, (src, ref) in enumerate(full)
                for i in range(4)
            ]

        def act(p):
            for i in range(4):
                dy_load(p, i).wait()
            for copy in gu_copies(p):
                copy.wait()
            if p > 0:
                for copy in out_copies(p - 1):
                    copy.wait()

            def tile(j, carry):
                count = tiles * p + j
                slot = lax.rem(count, 2)
                wd_copy(j, slot).wait()

                def ahead():
                    wd_copy(lax.rem(j + 1, tiles), 1 - slot).start()

                if p < 3:
                    ahead()
                else:
                    pl.when(j < tiles - 1)(ahead)
                if p == 0:

                    @pl.when((j > 0) & (j < 4))
                    def _():
                        for copy in w_copies(j - 1):
                            copy.start()

                at = pl.ds(pl.multiple_of(j * TILE, TILE), TILE)
                d_hidden = nt(dyc[...], wdb[slot])
                h, dg, du = act_and_back(gub[0, :, at], gub[1, :, at], d_hidden)
                dgc[p, :, at] = dg.astype(jnp.bfloat16)
                duc[p, :, at] = du.astype(jnp.bfloat16)
                hc[:, at] = h.astype(jnp.bfloat16)
                return carry

            lax.fori_loop(0, tiles, tile, 0)
            for copy in out_copies(p):
                copy.start()
            if p < 3:
                for copy in gu_copies(p + 1):
                    copy.start()

        def own_x(leg):
            hold = dgc.at[3, pl.ds(0, rows), :], duc.at[3, pl.ds(0, rows), :]
            cols = pl.ds(0, ff), pl.ds(ff, ff)
            return [
                pltpu.make_async_copy(
                    *((x_ref.at[:, cols[c]], hold[c]) if leg == 0 else (hold[c], xf_ref.at[block(me), cols[c]])),
                    own_sem.at[leg, c],
                )
                for c in range(2)
            ]

        def own_dy():
            return pltpu.make_async_copy(dyc.at[pl.ds(rows, rows), :], dyf_ref.at[block(me), :], own_sem.at[2, 0])

        dys.send(0, 1, 4, 2, 3)
        dy_load(0, 2).start()
        dy_load(0, 3).start()
        wd_copy(0, 0).start()
        for copy in gu_copies(0):
            copy.start()
        dys.arrived(0)
        dy_load(0, 0).start()
        dy_load(0, 1).start()
        for copy in own_x(0):
            copy.start()
        act(0)
        own_dy().start()
        for copy in own_x(0):
            copy.wait()
        for copy in own_x(1):
            copy.start()

        def first_halves():
            dys.arrived(1, 4)
            dys.send(5, 6, 13, 14, 7, 10)
            xs.send(0, 1, 4, 2, 3)

        def load(p, *numbers):
            def then():
                dys.arrived(*numbers)
                for i in range(4):
                    dy_load(p, i).start()

            return then

        def load_first():
            own_dy().wait()
            for copy in own_x(1):
                copy.wait()
            load(1, 7, 10)()

        def store_s(sums, _, outs):
            outs[0][...] = sums[0].astype(jnp.bfloat16)
            outs[1][...] = sums[1]

        dx(
            True, [(0, 0, rows), (0, rows, rows)], [], [give_ref.at[0], keep_s_ref], store_s,
            {wtiles - 3: first_halves, wtiles - 1: load_first},
        )
        pair(0).start()
        act(1)
        dys.arrived(2, 3)
        dys.send(8, 9)
        give(1, {wtiles - 1: load(2, 8, 9)})
        act(2)

        def far_halves():
            dys.arrived(5, 6, 13, 14)
            dys.send(11, 12, 15, 16)

        give(2, {wtiles - 4: far_halves, wtiles - 1: load(3, 11, 12, 15, 16)})
        act(3)

        def first_x_halves():
            xs.arrived(1, 4)
            xs.send(5, 6, 13, 14, 7, 10)

        give(3, {0: first_x_halves})
        for copy in out_copies(3):
            copy.wait()

    pl.run_scoped(
        with_acts,
        pltpu.VMEM((2 * rows, d), jnp.bfloat16),
        pltpu.VMEM((2, TILE, d), jnp.bfloat16),
        pltpu.VMEM((2, 2 * rows, ff), jnp.bfloat16),
        pltpu.VMEM((2 * rows, ff), jnp.bfloat16),
    )

    for p in (1, 2):
        pair(p).wait_recv()

    def second_halves():
        xs.arrived(2, 3)
        xs.send(8, 9)

    def store_near(sums, gots, outs):
        near0, near1 = (s + g[...].astype(jnp.float32) for s, g in zip(sums, gots))
        to_x, to_y, kept = outs
        to_x[...] = near0[:half].astype(jnp.bfloat16)
        to_y[...] = near0[half:].astype(jnp.bfloat16)
        kept[...] = near1

    dx(
        False, [(p, rows, rows) for p in (1, 2)], [got_ref.at[0], got_ref.at[1]],
        [send_x_ref.at[0], send_y_ref.at[0], keep_n_ref], store_near, {0: second_halves}, [half, half, rows],
    )
    pair(3).wait_recv()

    def store_far(sums, gots, outs):
        total = sums[0] + gots[0][...].astype(jnp.float32)
        outs[0][...] = total[:half].astype(jnp.bfloat16)
        outs[1][...] = total[half:].astype(jnp.bfloat16)

    dx(False, [(3, rows, rows)], [got_ref.at[2]], [send_x_ref.at[1], send_y_ref.at[1]], store_far, {}, [half, half])
    xs.arrived(5, 6)
    xs.send(11, 12)
    xs.arrived(13, 14)
    xs.send(15, 16)
    xs.arrived(0, 7, 8, 9, 10, 11, 12, 15, 16)
    pair(0).wait_recv()
    for p in range(4):
        pair(p).wait_send()
    dys.finish()
    xs.finish()


def front(dy, x, gate, up, wd, wg, wu):
    rows, d = dy.shape
    tokens, ff = gate.shape
    bf16, f32 = jnp.bfloat16, jnp.float32
    shapes = [
        ((tokens, d), bf16), ((tokens, d), bf16), ((tokens, ff), bf16), ((tokens, ff), bf16), ((tokens, ff), bf16),
        ((4, rows, d), bf16), ((rows, d), bf16), ((3, rows, d), bf16), ((rows, d), f32), ((rows, d), f32),
        ((2, rows // 2, d), bf16), ((2, rows // 2, d), bf16),
    ]
    dma = pltpu.SemaphoreType.DMA
    return pl.pallas_call(
        front_kernel,
        out_shape=[jax.ShapeDtypeStruct(*s) for s in shapes],
        in_specs=[ANY] * 7,
        out_specs=[ANY] * len(shapes),
        scratch_shapes=[
            pltpu.VMEM((4, 2 * rows, ff), bf16),
            pltpu.VMEM((4, 2 * rows, ff), bf16),
            pltpu.VMEM((2, d, ff), bf16),
            dma((2, 17)), dma((2, 17)), dma((4,)), dma((4,)), dma((d // WTILE, 2)),
            dma((4,)), dma((2,)), dma((2, 4)), dma((3, 4)), dma((3, 2)),
        ],
        compiler_params=pltpu.CompilerParams(
            collective_id=0, has_side_effects=True, vmem_limit_bytes=VMEM_LIMIT
        ),
        cost_estimate=pl.CostEstimate(
            flops=6 * tokens * d * ff, bytes_accessed=300 * 2**20, transcendentals=tokens * ff
        ),
        name="front",
    )(dy, x, gate, up, wd, wg, wu)


def dw_kernel(a_ref, b_ref, o_ref):
    o_ref[...] = tn(a_ref[...], b_ref[...]).astype(o_ref.dtype)


def dw(a, b, tm=512):
    tokens, m = a.shape
    n = b.shape[1]
    return pl.pallas_call(
        dw_kernel,
        out_shape=jax.ShapeDtypeStruct((m, n), jnp.bfloat16),
        grid=(m // tm,),
        in_specs=[
            pl.BlockSpec((tokens, tm), lambda i: (0, i)),
            pl.BlockSpec((tokens, n), lambda i: (0, 0), pipeline_mode=pl.Buffered(1)),
        ],
        out_specs=pl.BlockSpec((tm, n), lambda i: (i, 0)),
        compiler_params=pltpu.CompilerParams(dimension_semantics=("arbitrary",), vmem_limit_bytes=52 * 2**20),
        cost_estimate=pl.CostEstimate(
            flops=2 * tokens * m * n, bytes_accessed=2 * (tokens * m + tokens * n + m * n), transcendentals=0
        ),
        name="dw",
    )(a, b)


def dw_two(h, dy, x, dg, tile=512):
    tokens, ff = h.shape
    d = dy.shape[1]
    steps = d // tile

    def kernel(dy_ref, x_ref, h_hbm, dg_hbm, down_ref, gate_ref, h_held, held, h_sem, sem):
        i = pl.program_id(0)
        load = pltpu.make_async_copy(dg_hbm, held, sem)
        cuts = [pl.ds(c, 256) for c in range(0, ff, 256)]
        pieces = [pltpu.make_async_copy(h_hbm.at[:, at], h_held.at[:, at], h_sem.at[j]) for j, at in enumerate(cuts)]

        @pl.when(i == 0)
        def _():
            for piece in pieces:
                piece.start()
            load.start()
            for piece, at in zip(pieces, cuts):
                piece.wait()
                down_ref[at, :] = tn(h_held[:, at], dy_ref[...]).astype(down_ref.dtype)

        @pl.when((i > 0) & (i < steps))
        def _():
            down_ref[...] = tn(h_held[...], dy_ref[...]).astype(down_ref.dtype)

        @pl.when(i == steps - 1)
        def _():
            load.wait()

        @pl.when(i >= steps)
        def _():
            gate_ref[...] = tn(x_ref[...], held[...]).astype(gate_ref.dtype)

    def first(i):
        return jnp.minimum(i, steps - 1)

    def second(i):
        return jnp.maximum(i - steps, 0)

    return pl.pallas_call(
        kernel,
        out_shape=[jax.ShapeDtypeStruct((ff, d), jnp.bfloat16), jax.ShapeDtypeStruct((d, ff), jnp.bfloat16)],
        grid=(2 * steps,),
        in_specs=[
            pl.BlockSpec((tokens, tile), lambda i: (0, first(i))),
            pl.BlockSpec((tokens, tile), lambda i: (0, second(i))),
            ANY,
            ANY,
        ],
        out_specs=[
            pl.BlockSpec((ff, tile), lambda i: (0, first(i))),
            pl.BlockSpec((tile, ff), lambda i: (second(i), 0)),
        ],
        scratch_shapes=[
            pltpu.VMEM((tokens, ff), jnp.bfloat16),
            pltpu.VMEM((tokens, ff), jnp.bfloat16),
            pltpu.SemaphoreType.DMA((ff // 256,)),
            pltpu.SemaphoreType.DMA(()),
        ],
        compiler_params=pltpu.CompilerParams(dimension_semantics=("arbitrary",), vmem_limit_bytes=48 * 2**20),
        cost_estimate=pl.CostEstimate(
            flops=4 * tokens * d * ff, bytes_accessed=4 * (tokens * d + tokens * ff + d * ff), transcendentals=0
        ),
        name="dw_two",
    )(dy, x, h, dg)


def sum_on(kept, from_x, from_y, tile=1792):
    rows, d = kept.shape
    half = rows // 2

    def kernel(kept_ref, fx_ref, fy_ref, ony_ref, onx_ref):
        onx_ref[...] = (kept_ref[pl.ds(0, half), :] + fy_ref[0].astype(jnp.float32)).astype(jnp.bfloat16)
        ony_ref[...] = (kept_ref[pl.ds(half, half), :] + fx_ref[0].astype(jnp.float32)).astype(jnp.bfloat16)

    part = pl.BlockSpec((1, half, tile), lambda i: (1, 0, i))
    out = pl.BlockSpec((half, tile), lambda i: (0, i))
    return pl.pallas_call(
        kernel,
        out_shape=[jax.ShapeDtypeStruct((half, d), jnp.bfloat16)] * 2,
        grid=(d // tile,),
        in_specs=[pl.BlockSpec((rows, tile), lambda i: (0, i)), part, part],
        out_specs=[out, out],
        compiler_params=pltpu.CompilerParams(dimension_semantics=("arbitrary",), vmem_limit_bytes=20 * 2**20),
        cost_estimate=pl.CostEstimate(flops=rows * d, bytes_accessed=8 * rows * d, transcendentals=0),
        name="sum_on",
    )(kept, from_x, from_y)


def sum_rows(kept, got, from_x, from_y, last_x, last_y, tile=896):
    rows, d = kept.shape
    half = rows // 2

    def kernel(kept_ref, got_ref, fx_ref, fy_ref, lx_ref, ly_ref, o_ref):
        f32 = jnp.float32
        for at, near, last in ((pl.ds(0, half), fx_ref, ly_ref), (pl.ds(half, half), fy_ref, lx_ref)):
            total = kept_ref[at, :] + got_ref[at, :].astype(f32) + near[0].astype(f32) + last[...].astype(f32)
            o_ref[at, :] = total.astype(o_ref.dtype)

    full = pl.BlockSpec((rows, tile), lambda i: (0, i))
    part = pl.BlockSpec((1, half, tile), lambda i: (0, 0, i))
    last = pl.BlockSpec((half, tile), lambda i: (0, i))
    return pl.pallas_call(
        kernel,
        out_shape=jax.ShapeDtypeStruct((rows, d), jnp.bfloat16),
        grid=(d // tile,),
        in_specs=[full, full, part, part, last, last],
        out_specs=full,
        compiler_params=pltpu.CompilerParams(dimension_semantics=("arbitrary",), vmem_limit_bytes=20 * 2**20),
        cost_estimate=pl.CostEstimate(flops=4 * rows * d, bytes_accessed=14 * rows * d, transcendentals=0),
        name="sum_rows",
    )(kept, got, from_x, from_y, last_x, last_y)


def solution(mesh):
    devices = mesh.shape["tp"]
    to_x = [(i, i ^ 4) for i in range(devices)]
    to_y = [(i, i ^ 2) for i in range(devices)]

    def step(x, dy, gate, up, wg, wu, wd):
        dyf, xf, dg, du, h, _, got_s, _, keep_s, keep_n, send_x, send_y = front(dy, x, gate, up, wd, wg, wu)
        from_x = lax.ppermute(send_x, "tp", to_x)
        from_y = lax.ppermute(send_y, "tp", to_y)
        dw_down, dw_gate = dw_two(h, dyf, xf, dg)
        on_y, on_x = sum_on(keep_n, from_x, from_y)
        du, on_y, on_x = lax.optimization_barrier((du, on_y, on_x))
        last_y = lax.ppermute(on_y, "tp", to_y)
        last_x = lax.ppermute(on_x, "tp", to_x)
        dw_up = dw(xf, du)
        dx = sum_rows(keep_s, got_s, from_x, from_y, last_x, last_y)
        return dx, dw_gate, dw_up, dw_down

    rows, cols, down = P(("dp", "tp"), None), P("dp", "tp"), P("tp", None)
    weight = P(None, "tp")
    return jax.shard_map(
        step,
        mesh=mesh,
        in_specs=(rows, rows, cols, cols, weight, weight, down),
        out_specs=(rows, cols, cols, P(("dp", "tp"), None)),
        check_vma=False,
    )
```

```python
import jax
import jax.numpy as jnp
from jax import lax
from jax.experimental import pallas as pl
from jax.experimental.pallas import tpu as pltpu
from jax.sharding import PartitionSpec as P

MESH = pl.DeviceIdType.MESH
ANY = pl.BlockSpec(memory_space=pl.ANY)
VMEM_LIMIT = 67043328
C0 = 0.7978845608028654
C1 = C0 * 0.044715


def act_and_back(gate, up, d_hidden):
    g = gate.astype(jnp.float32)
    u = up.astype(jnp.float32)
    g2 = g * g
    t = jnp.tanh(g * (C0 + C1 * g2))
    cdf = 0.5 + 0.5 * t
    gelu = g * cdf
    slope = cdf + (0.5 * g) * (1.0 - t * t) * (C0 + (3.0 * C1) * g2)
    return gelu * u, d_hidden * u * slope, d_hidden * gelu


def nt(a, b):
    return lax.dot_general(a, b, (((1,), (1,)), ((), ())), preferred_element_type=jnp.float32)


def tn(a, b):
    return lax.dot_general(a, b, (((0,), (0,)), ((), ())), preferred_element_type=jnp.float32)

TILE = 256
WTILE = 512


def front_kernel(
    dy_ref, x_ref, gate_ref, up_ref, wd_ref, wg_ref, wu_ref,
    dyf_ref, xf_ref, dg_ref, du_ref, h_ref, give_ref, got_s_ref, got_ref, keep_s_ref, keep_n_ref, send_x_ref, send_y_ref,
    dgc, duc, wbuf, send_sem, recv_sem, pair_send, pair_recv, w_sem, dy_sem, wd_sem, gu_sem, out_sem, own_sem,
):
    rows, d = dy_ref.shape
    half = rows // 2
    ff = wd_ref.shape[0]
    tiles, wtiles = ff // TILE, d // WTILE
    me = lax.axis_index("tp")
    other = me + 1 - 2 * (me % 2)
    near_y = me + 2 - 4 * ((me // 2) % 2)
    near_x = me + 4 - 8 * (me // 4)
    far = near_y + 4 - 8 * (near_y // 4)
    across = other - me

    barrier = pltpu.get_barrier_semaphore()
    for peer in (other, near_y, near_x):
        pl.semaphore_signal(barrier, inc=1, device_id={"tp": peer}, device_id_type=MESH)
    pl.semaphore_wait(barrier, 3)

    def block(owner, part=None):
        if part is None:
            return pl.ds(pl.multiple_of(owner * rows, rows), rows)
        return pl.ds(pl.multiple_of(owner * rows + part * half, half), half)

    routes = [
        (me, None, other),
        (me, 0, near_x), (me, 1, near_x), (me, 0, near_y), (me, 1, near_y),
        (near_x, 0, near_y), (near_y, 1, near_x),
        (near_x, 0, other), (near_x, 1, other), (near_y, 0, other), (near_y, 1, other),
        (far, 0, other), (far, 1, other),
    ]
    places = [block(owner, part) for owner, part, _ in routes]

    class Gather:
        def __init__(self, a, own, full):
            self.a, self.own, self.full = a, own, full

        def copy(self, number):
            _, part, peer = routes[number]
            if number < 5:
                src = self.own if part is None else self.own.at[pl.ds(part * half, half), :]
            else:
                src = self.full.at[places[number], :]
            return pltpu.make_async_remote_copy(
                src_ref=src,
                dst_ref=self.full.at[places[number], :],
                send_sem=send_sem.at[self.a, number],
                recv_sem=recv_sem.at[self.a, number],
                device_id={"tp": peer},
                device_id_type=MESH,
            )

        def send(self, *numbers):
            for number in numbers:
                self.copy(number).start()

        def arrived(self, *numbers):
            for number in numbers:
                self.copy(number).wait_recv()

        def finish(self):
            for number in range(len(routes)):
                self.copy(number).wait_send()

    dys, xs = Gather(0, dy_ref, dyf_ref), Gather(1, x_ref, xf_ref)

    def pair(p):
        return pltpu.make_async_remote_copy(
            src_ref=give_ref.at[p],
            dst_ref=got_s_ref if p == 0 else got_ref.at[p - 1],
            send_sem=pair_send.at[p],
            recv_sem=pair_recv.at[p],
            device_id={"tp": other},
            device_id_type=MESH,
        )

    pieces = [
        [(other, 0), (other, 1), (me, 0), (me, 1)],
        [(near_x + across, 0), (near_y + across, 1), (near_x, 0), (near_y, 1)],
        [(near_x + across, 1), (near_y + across, 0), (near_x, 1), (near_y, 0)],
        [(far + across, 0), (far + across, 1), (far, 0), (far, 1)],
    ]
    where = [[block(*piece) for piece in part] for part in pieces]

    def w_rows(tile):
        return pl.ds(pl.multiple_of(tile * WTILE, WTILE), WTILE)

    def w_copies(tile):
        at = w_rows(tile)
        return [
            pltpu.make_async_copy(ref.at[at, :], wbuf.at[i, at, :], w_sem.at[tile, i]) for i, ref in enumerate((wg_ref, wu_ref))
        ]

    def dx(first_pass, parts, ins, outs, store, hooks, heights=None):
        def body(step, *refs):
            n = step.index[0]
            at = w_rows(n)
            if first_pass:
                for copy in w_copies(n):
                    copy.wait()

                @pl.when(n + 3 < wtiles)
                def _():
                    for copy in w_copies(n + 3):
                        copy.start()

            for when, hook in hooks.items():
                pl.when(n == when)(hook)
            sums = [
                nt(dgc[p, pl.ds(first, count), :], wbuf[0, at, :]) + nt(duc[p, pl.ds(first, count), :], wbuf[1, at, :])
                for p, first, count in parts
            ]
            store(sums, refs[: len(ins)], refs[len(ins) :])

        def spec(height):
            return pl.BlockSpec((height, WTILE), lambda n: (0, n))

        pltpu.emit_pipeline(
            body,
            grid=(wtiles,),
            in_specs=[spec(rows) for _ in ins],
            out_specs=[spec(height) for height in heights or [rows] * len(outs)],
            _explicit_indices=True,
        )(*ins, *outs)

    def give(p, hooks={}):
        def store(sums, _, outs):
            outs[0][...] = sums[0].astype(jnp.bfloat16)

        dx(False, [(p, 0, rows)], [], [give_ref.at[p]], store, hooks)
        pair(p).start()

    def with_acts(dyc, wdb, gub, hc):
        def dy_load(p, i):
            if p == 0 and i >= 2:
                src = dy_ref.at[pl.ds((i - 2) * half, half), :]
            else:
                src = dyf_ref.at[where[p][i], :]
            return pltpu.make_async_copy(src, dyc.at[pl.ds(i * half, half), :], dy_sem.at[i])

        def wd_copy(j, slot):
            at = pl.ds(pl.multiple_of(j * TILE, TILE), TILE)
            return pltpu.make_async_copy(wd_ref.at[at, :], wdb.at[slot], wd_sem.at[slot])

        def gu_copies(p):
            return [
                pltpu.make_async_copy(ref.at[where[p][i], :], gub.at[j, pl.ds(i * half, half), :], gu_sem.at[j, i])
                for j, ref in enumerate((gate_ref, up_ref))
                for i in range(4)
            ]

        def out_copies(p):
            full = ((dgc.at[p], dg_ref), (duc.at[p], du_ref), (hc, h_ref))
            return [
                pltpu.make_async_copy(src.at[pl.ds(i * half, half), :], ref.at[where[p][i], :], out_sem.at[j, i])
                for j, (src, ref) in enumerate(full)
                for i in range(4)
            ]

        def act(p):
            for i in range(4):
                dy_load(p, i).wait()
            for copy in gu_copies(p):
                copy.wait()
            if p > 0:
                for copy in out_copies(p - 1):
                    copy.wait()

            def tile(j, carry):
                count = tiles * p + j
                slot = lax.rem(count, 2)
                wd_copy(j, slot).wait()

                def ahead():
                    wd_copy(lax.rem(j + 1, tiles), 1 - slot).start()

                if p < 3:
                    ahead()
                else:
                    pl.when(j < tiles - 1)(ahead)
                if p == 0:

                    @pl.when((j > 0) & (j < 4))
                    def _():
                        for copy in w_copies(j - 1):
                            copy.start()

                at = pl.ds(pl.multiple_of(j * TILE, TILE), TILE)
                d_hidden = nt(dyc[...], wdb[slot])
                h, dg, du = act_and_back(gub[0, :, at], gub[1, :, at], d_hidden)
                dgc[p, :, at] = dg.astype(jnp.bfloat16)
                duc[p, :, at] = du.astype(jnp.bfloat16)
                hc[:, at] = h.astype(jnp.bfloat16)
                return carry

            lax.fori_loop(0, tiles, tile, 0)
            for copy in out_copies(p):
                copy.start()
            if p < 3:
                for copy in gu_copies(p + 1):
                    copy.start()

        def own_x(leg):
            hold = dgc.at[3, pl.ds(0, rows), :], duc.at[3, pl.ds(0, rows), :]
            cols = pl.ds(0, ff), pl.ds(ff, ff)
            return [
                pltpu.make_async_copy(
                    *((x_ref.at[:, cols[c]], hold[c]) if leg == 0 else (hold[c], xf_ref.at[block(me), cols[c]])),
                    own_sem.at[leg, c],
                )
                for c in range(2)
            ]

        def own_dy():
            return pltpu.make_async_copy(dyc.at[pl.ds(rows, rows), :], dyf_ref.at[block(me), :], own_sem.at[2, 0])

        dys.send(0, 1, 4, 2, 3)
        dy_load(0, 2).start()
        dy_load(0, 3).start()
        wd_copy(0, 0).start()
        for copy in gu_copies(0):
            copy.start()
        dys.arrived(0)
        dy_load(0, 0).start()
        dy_load(0, 1).start()
        for copy in own_x(0):
            copy.start()
        act(0)
        own_dy().start()
        for copy in own_x(0):
            copy.wait()
        for copy in own_x(1):
            copy.start()

        def first_halves():
            dys.arrived(1, 4)
            dys.send(5, 6, 7, 10)
            xs.send(0, 1, 4, 2, 3)

        def load(p, *numbers):
            def then():
                dys.arrived(*numbers)
                for i in range(4):
                    dy_load(p, i).start()

            return then

        def load_first():
            own_dy().wait()
            for copy in own_x(1):
                copy.wait()
            load(1, 7, 10)()

        def store_s(sums, _, outs):
            outs[0][...] = sums[0].astype(jnp.bfloat16)
            outs[1][...] = sums[1]

        dx(
            True, [(0, 0, rows), (0, rows, rows)], [], [give_ref.at[0], keep_s_ref], store_s,
            {wtiles - 3: first_halves, wtiles - 1: load_first},
        )
        pair(0).start()
        act(1)
        dys.arrived(2, 3)
        dys.send(8, 9)
        give(1, {wtiles - 1: load(2, 8, 9)})
        act(2)

        def far_halves():
            dys.arrived(5, 6)
            dys.send(11, 12)

        give(2, {wtiles - 4: far_halves, wtiles - 1: load(3, 11, 12)})
        act(3)

        def first_x_halves():
            xs.arrived(1, 4)
            xs.send(5, 6, 7, 10)

        give(3, {0: first_x_halves})
        for copy in out_copies(3):
            copy.wait()

    pl.run_scoped(
        with_acts,
        pltpu.VMEM((2 * rows, d), jnp.bfloat16),
        pltpu.VMEM((2, TILE, d), jnp.bfloat16),
        pltpu.VMEM((2, 2 * rows, ff), jnp.bfloat16),
        pltpu.VMEM((2 * rows, ff), jnp.bfloat16),
    )

    for p in (1, 2):
        pair(p).wait_recv()

    def second_halves():
        xs.arrived(2, 3)
        xs.send(8, 9)

    def store_near(sums, gots, outs):
        near0, near1 = (s + g[...].astype(jnp.float32) for s, g in zip(sums, gots))
        to_x, to_y, kept = outs
        to_x[...] = near0[:half].astype(jnp.bfloat16)
        to_y[...] = near0[half:].astype(jnp.bfloat16)
        kept[...] = near1

    dx(
        False, [(p, rows, rows) for p in (1, 2)], [got_ref.at[0], got_ref.at[1]],
        [send_x_ref.at[0], send_y_ref.at[0], keep_n_ref], store_near, {0: second_halves}, [half, half, rows],
    )
    pair(3).wait_recv()

    def store_far(sums, gots, outs):
        total = sums[0] + gots[0][...].astype(jnp.float32)
        outs[0][...] = total[:half].astype(jnp.bfloat16)
        outs[1][...] = total[half:].astype(jnp.bfloat16)

    dx(False, [(3, rows, rows)], [got_ref.at[2]], [send_x_ref.at[1], send_y_ref.at[1]], store_far, {}, [half, half])
    xs.arrived(5, 6)
    xs.send(11, 12)
    xs.arrived(0, 7, 8, 9, 10, 11, 12)
    pair(0).wait_recv()
    for p in range(4):
        pair(p).wait_send()
    dys.finish()
    xs.finish()


def front(dy, x, gate, up, wd, wg, wu):
    rows, d = dy.shape
    tokens, ff = gate.shape
    bf16, f32 = jnp.bfloat16, jnp.float32
    shapes = [
        ((tokens, d), bf16), ((tokens, d), bf16), ((tokens, ff), bf16), ((tokens, ff), bf16), ((tokens, ff), bf16),
        ((4, rows, d), bf16), ((rows, d), bf16), ((3, rows, d), bf16), ((rows, d), f32), ((rows, d), f32),
        ((2, rows // 2, d), bf16), ((2, rows // 2, d), bf16),
    ]
    dma = pltpu.SemaphoreType.DMA
    return pl.pallas_call(
        front_kernel,
        out_shape=[jax.ShapeDtypeStruct(*s) for s in shapes],
        in_specs=[ANY] * 7,
        out_specs=[ANY] * len(shapes),
        scratch_shapes=[
            pltpu.VMEM((4, 2 * rows, ff), bf16),
            pltpu.VMEM((4, 2 * rows, ff), bf16),
            pltpu.VMEM((2, d, ff), bf16),
            dma((2, 13)), dma((2, 13)), dma((4,)), dma((4,)), dma((d // WTILE, 2)),
            dma((4,)), dma((2,)), dma((2, 4)), dma((3, 4)), dma((3, 2)),
        ],
        compiler_params=pltpu.CompilerParams(
            collective_id=0, has_side_effects=True, vmem_limit_bytes=VMEM_LIMIT
        ),
        cost_estimate=pl.CostEstimate(
            flops=6 * tokens * d * ff, bytes_accessed=300 * 2**20, transcendentals=tokens * ff
        ),
        name="front",
    )(dy, x, gate, up, wd, wg, wu)


def dw_kernel(a_ref, b_ref, o_ref):
    o_ref[...] = tn(a_ref[...], b_ref[...]).astype(o_ref.dtype)


def dw(a, b, tm=512):
    tokens, m = a.shape
    n = b.shape[1]
    return pl.pallas_call(
        dw_kernel,
        out_shape=jax.ShapeDtypeStruct((m, n), jnp.bfloat16),
        grid=(m // tm,),
        in_specs=[
            pl.BlockSpec((tokens, tm), lambda i: (0, i)),
            pl.BlockSpec((tokens, n), lambda i: (0, 0), pipeline_mode=pl.Buffered(1)),
        ],
        out_specs=pl.BlockSpec((tm, n), lambda i: (i, 0)),
        compiler_params=pltpu.CompilerParams(dimension_semantics=("arbitrary",), vmem_limit_bytes=52 * 2**20),
        cost_estimate=pl.CostEstimate(
            flops=2 * tokens * m * n, bytes_accessed=2 * (tokens * m + tokens * n + m * n), transcendentals=0
        ),
        name="dw",
    )(a, b)


def dw_two(h, dy, x, dg, tile=512):
    tokens, ff = h.shape
    d = dy.shape[1]
    steps = d // tile

    def kernel(dy_ref, x_ref, h_hbm, dg_hbm, down_ref, gate_ref, h_held, held, h_sem, sem):
        i = pl.program_id(0)
        load = pltpu.make_async_copy(dg_hbm, held, sem)
        cuts = [pl.ds(c, 256) for c in range(0, ff, 256)]
        pieces = [pltpu.make_async_copy(h_hbm.at[:, at], h_held.at[:, at], h_sem.at[j]) for j, at in enumerate(cuts)]

        @pl.when(i == 0)
        def _():
            for piece in pieces:
                piece.start()
            load.start()
            for piece, at in zip(pieces, cuts):
                piece.wait()
                down_ref[at, :] = tn(h_held[:, at], dy_ref[...]).astype(down_ref.dtype)

        @pl.when((i > 0) & (i < steps))
        def _():
            down_ref[...] = tn(h_held[...], dy_ref[...]).astype(down_ref.dtype)

        @pl.when(i == steps - 1)
        def _():
            load.wait()

        @pl.when(i >= steps)
        def _():
            gate_ref[...] = tn(x_ref[...], held[...]).astype(gate_ref.dtype)

    def first(i):
        return jnp.minimum(i, steps - 1)

    def second(i):
        return jnp.maximum(i - steps, 0)

    return pl.pallas_call(
        kernel,
        out_shape=[jax.ShapeDtypeStruct((ff, d), jnp.bfloat16), jax.ShapeDtypeStruct((d, ff), jnp.bfloat16)],
        grid=(2 * steps,),
        in_specs=[
            pl.BlockSpec((tokens, tile), lambda i: (0, first(i))),
            pl.BlockSpec((tokens, tile), lambda i: (0, second(i))),
            ANY,
            ANY,
        ],
        out_specs=[
            pl.BlockSpec((ff, tile), lambda i: (0, first(i))),
            pl.BlockSpec((tile, ff), lambda i: (second(i), 0)),
        ],
        scratch_shapes=[
            pltpu.VMEM((tokens, ff), jnp.bfloat16),
            pltpu.VMEM((tokens, ff), jnp.bfloat16),
            pltpu.SemaphoreType.DMA((ff // 256,)),
            pltpu.SemaphoreType.DMA(()),
        ],
        compiler_params=pltpu.CompilerParams(dimension_semantics=("arbitrary",), vmem_limit_bytes=48 * 2**20),
        cost_estimate=pl.CostEstimate(
            flops=4 * tokens * d * ff, bytes_accessed=4 * (tokens * d + tokens * ff + d * ff), transcendentals=0
        ),
        name="dw_two",
    )(dy, x, h, dg)


def sum_on(kept, from_x, from_y, tile=1792):
    rows, d = kept.shape
    half = rows // 2

    def kernel(kept_ref, fx_ref, fy_ref, ony_ref, onx_ref):
        onx_ref[...] = (kept_ref[pl.ds(0, half), :] + fy_ref[0].astype(jnp.float32)).astype(jnp.bfloat16)
        ony_ref[...] = (kept_ref[pl.ds(half, half), :] + fx_ref[0].astype(jnp.float32)).astype(jnp.bfloat16)

    part = pl.BlockSpec((1, half, tile), lambda i: (1, 0, i))
    out = pl.BlockSpec((half, tile), lambda i: (0, i))
    return pl.pallas_call(
        kernel,
        out_shape=[jax.ShapeDtypeStruct((half, d), jnp.bfloat16)] * 2,
        grid=(d // tile,),
        in_specs=[pl.BlockSpec((rows, tile), lambda i: (0, i)), part, part],
        out_specs=[out, out],
        compiler_params=pltpu.CompilerParams(dimension_semantics=("arbitrary",), vmem_limit_bytes=20 * 2**20),
        cost_estimate=pl.CostEstimate(flops=rows * d, bytes_accessed=8 * rows * d, transcendentals=0),
        name="sum_on",
    )(kept, from_x, from_y)


def sum_rows(kept, got, from_x, from_y, last_x, last_y):
    rows, d = kept.shape
    half = rows // 2

    def kernel(kept_ref, got_ref, fx_ref, fy_ref, lx_ref, ly_ref, o_ref):
        f32 = jnp.float32
        for at, near, last in ((pl.ds(0, half), fx_ref, ly_ref), (pl.ds(half, half), fy_ref, lx_ref)):
            total = kept_ref[at, :] + got_ref[at, :].astype(f32) + near[0].astype(f32) + last[...].astype(f32)
            o_ref[at, :] = total.astype(o_ref.dtype)

    return pl.pallas_call(
        kernel,
        out_shape=jax.ShapeDtypeStruct((rows, d), jnp.bfloat16),
        in_specs=[pl.BlockSpec(memory_space=pltpu.VMEM)] * 6,
        out_specs=pl.BlockSpec(memory_space=pltpu.VMEM),
        compiler_params=pltpu.CompilerParams(vmem_limit_bytes=20 * 2**20),
        cost_estimate=pl.CostEstimate(flops=4 * rows * d, bytes_accessed=14 * rows * d, transcendentals=0),
        name="sum_rows",
    )(kept, got, from_x, from_y, last_x, last_y)


def solution(mesh):
    devices = mesh.shape["tp"]
    to_x = [(i, i ^ 4) for i in range(devices)]
    to_y = [(i, i ^ 2) for i in range(devices)]

    def step(x, dy, gate, up, wg, wu, wd):
        dyf, xf, dg, du, h, _, got_s, _, keep_s, keep_n, send_x, send_y = front(dy, x, gate, up, wd, wg, wu)
        from_x = lax.ppermute(send_x, "tp", to_x)
        from_y = lax.ppermute(send_y, "tp", to_y)
        dw_down, dw_gate = dw_two(h, dyf, xf, dg)
        on_y, on_x = sum_on(keep_n, from_x, from_y)
        du, on_y, on_x = lax.optimization_barrier((du, on_y, on_x))
        last_y = lax.ppermute(on_y, "tp", to_y)
        last_x = lax.ppermute(on_x, "tp", to_x)
        dw_up = dw(xf, du)
        dx = sum_rows(keep_s, got_s, from_x, from_y, last_x, last_y)
        return dx, dw_gate, dw_up, dw_down

    rows, cols, down = P(("dp", "tp"), None), P("dp", "tp"), P("tp", None)
    weight = P(None, "tp")
    return jax.shard_map(
        step,
        mesh=mesh,
        in_specs=(rows, rows, cols, cols, weight, weight, down),
        out_specs=(rows, cols, cols, P(("dp", "tp"), None)),
        check_vma=False,
    )
```
